32 devices in a mesh: gx: 8 (over z, x), gy: 4 (over y, core).
Axes of the slice: x: 2, y: 2, z: 4, core: 2. Of those that a mesh axis runs over, the one named last changes fastest.
Arguments:
- state: float32 [65536, 128], P(('gx', 'gy')), may hold values from 0 to 1
- velocity: bfloat16 [3, 3, 128, 64, 128], P(None, None, 'gx', 'gy'), may hold values from -3 to 3
- cells: int32 [3, 3, 65536], P(None, None, ('gx', 'gy')), may hold values from -1 to 126, as said below
- slots: int32 [3, 65536], P(None, ('gx', 'gy')), may hold values from 0 to 2047, as said below
- counts: int32 [3, 8, 4, 8], P(None, 'gx', 'gy'), may hold values from 0 to 64, as said below
Outputs:
- final_state: float32 [65536, 128], P(('gx', 'gy'))
The draws below stay inside these ranges and needn't reach their ends.
Inputs may be any that keep to these rules, and one draw needn't show every extreme that they name: For every section and device the 2048 values of slots are a permutation of 0 to 2047. counts[s, i, j, r] equals counts[s, i', j', r xor 1] where (i', j') is the neighbour of (i, j) in direction r; some device sends exactly 64 in every section. cells[s, 0] lies in -1 to 15, cells[s, 1] in -1 to 15, cells[s, 2] in 0 to 126.
All inputs are finite; a program needn't handle non-finite values.
Results may differ from the reference program's by a relative error of at most 0.0003.
Values may be sent and summed in bfloat16 or wider, within the bound.
No kernel may reach another device: no remote copies, remote signals or barrier semaphores. Data moves between devices by JAX's collectives and lax.ppermute only.
A program may use at most 64 MiB of HBM per device.

```python
import jax
import jax.numpy as jnp

CX = 16
CY = 16
NZ = 128
PART_DEV = 2048
CAP = 64
S = 128
SECTIONS = 3
NX = 128
NY = 64
NPART = 65536
N_GX = 8
N_GY = 4


def draw_counts(key, part):
    forward = jax.random.randint(key, (SECTIONS, N_GX, N_GY, 4), CAP // 4, CAP + 1)
    picks = jax.random.randint(jax.random.fold_in(key, 7), (SECTIONS,), 0, N_GX * N_GY)
    hot = (jnp.arange(N_GX * N_GY)[None, :] == picks[:, None]).reshape(SECTIONS, N_GX, N_GY)
    east = jnp.where(hot, CAP, forward[..., 0])
    north = forward[..., 1]
    rising = forward[..., 2]
    falling = forward[..., 3]
    table = jnp.stack([east, jnp.roll(east, 1, axis=1), north, jnp.roll(north, 1, axis=2), rising, jnp.roll(rising, (1, 1), axis=(1, 2)), falling, jnp.roll(falling, (1, -1), axis=(1, 2))], axis=-1)
    return table.astype(jnp.int32)


def draw_slots(key, part):
    scores = jax.random.randint(key, (SECTIONS, N_GX * N_GY, PART_DEV), 0, 2 ** 18)
    scores = scores * PART_DEV + jnp.arange(PART_DEV, dtype=jnp.int32)[None, None, :]
    order = jnp.argsort(scores, axis=-1, stable=True).astype(jnp.int32)
    return order.reshape(SECTIONS, N_GX * N_GY * PART_DEV)


def draw_cells(key, part):
    npart = N_GX * N_GY * PART_DEV
    cell_x = jax.random.randint(jax.random.fold_in(key, 1), (SECTIONS, npart), -1, CX)
    cell_y = jax.random.randint(jax.random.fold_in(key, 2), (SECTIONS, npart), -1, CY)
    cell_z = jax.random.randint(jax.random.fold_in(key, 3), (SECTIONS, npart), 0, NZ - 1)
    return jnp.stack([cell_x, cell_y, cell_z], axis=1).astype(jnp.int32)


def level_of(key, shape, split, low, top_value):
    gain = 1.0
    for position, parts in split:
        draws = jax.random.uniform(jax.random.fold_in(jax.random.fold_in(key, 6), position), (parts,), jnp.float32, low / len(split), top_value / len(split))
        gain = gain * jnp.repeat(jnp.exp(draws), shape[position] // parts).reshape((-1,) + (1,) * (len(shape) - 1 - position))
    return gain


def normal_values(own_key, dims, scale, reach, pieces=(), held_as=jnp.bfloat16):
    gain = level_of(own_key, dims, pieces, -0.22, 0.18) if pieces else 1.0
    array = jax.random.normal(own_key, dims, jnp.float32) * scale * gain
    return jnp.minimum(jnp.maximum(array, -reach), reach).astype(held_as)


def setup_inputs(seed: int = 0) -> dict:
    key_of = jax.random.split(jax.random.key(seed), 6)
    state = jnp.clip(1.0 * jax.random.uniform(key_of[0], (NPART, S), jnp.float32) ** level_of(key_of[0], (NPART, S), ((0, 32),), -0.2, 0.2), 0.0, 1.0)
    velocity = normal_values(key_of[1], (SECTIONS, 3, NX, NY, NZ), 0.4, 3.0, ((2, 8), (3, 4)))
    cells = draw_cells(jax.random.fold_in(key_of[5], 71), 0)
    slots = draw_slots(jax.random.fold_in(key_of[5], 71), 0)
    counts = draw_counts(jax.random.fold_in(key_of[5], 71), 0)
    return dict(state=state, velocity=velocity, cells=cells, slots=slots, counts=counts)


GAMMA = (8.0 / 15.0, 5.0 / 12.0, 3.0 / 4.0)
ZETA = (0.0, -17.0 / 60.0, -5.0 / 12.0)
OFFSETS = ((1, 0), (-1, 0), (0, 1), (0, -1), (1, 1), (-1, -1), (1, -1), (-1, 1))
OPPOSITE = (1, 0, 3, 2, 5, 4, 7, 6)


def reference(state, velocity, cells, slots, counts):
    devices = N_GX * N_GY
    npart = devices * PART_DEV
    owner = jnp.arange(npart, dtype=jnp.int32) // PART_DEV
    row_i = owner // N_GY
    col_j = owner % N_GY
    lanes = jnp.arange(devices, dtype=jnp.int32)
    lane_i = lanes // N_GY
    lane_j = lanes % N_GY
    within = jnp.arange(CAP, dtype=jnp.int32)
    for section in range(SECTIONS):
        field = velocity[section]
        base_x = row_i * CX + cells[section, 0]
        base_y = col_j * CY + cells[section, 1]
        base_z = cells[section, 2]
        frac = state[:, 0:3]
        sampled = jnp.zeros((3, npart), jnp.float32)
        for a in (0, 1):
            for b in (0, 1):
                for c in (0, 1):
                    weight_x = frac[:, 0] if a else 1.0 - frac[:, 0]
                    weight_y = frac[:, 1] if b else 1.0 - frac[:, 1]
                    weight_z = frac[:, 2] if c else 1.0 - frac[:, 2]
                    index_x = (base_x + a) % NX
                    index_y = (base_y + b) % NY
                    values = field[:, index_x, index_y, base_z + c].astype(jnp.float32)
                    sampled = sampled + (weight_x * weight_y * weight_z)[None, :] * values
        speed = sampled.T
        moved = frac + GAMMA[section] * speed + ZETA[section] * state[:, 3:6]
        state = jnp.concatenate([moved, speed, state[:, 6:]], axis=1)
        order = slots[section].reshape(devices, PART_DEV)
        tally = counts[section].reshape(devices, 8)
        source = jnp.arange(npart, dtype=jnp.int32)
        for direction in range(8):
            off_x, off_y = OFFSETS[direction]
            back = OPPOSITE[direction]
            neighbour = ((lane_i + off_x) % N_GX) * N_GY + (lane_j + off_y) % N_GY
            far = neighbour[:, None] * PART_DEV + order[neighbour, back * CAP:(back + 1) * CAP]
            near = lanes[:, None] * PART_DEV + order[:, direction * CAP:(direction + 1) * CAP]
            picked = jnp.where(within[None, :] < tally[:, direction:direction + 1], far, near)
            source = source.at[near.reshape(-1)].set(picked.reshape(-1).astype(jnp.int32))
        state = state[source]
    return state
```

```python
import functools

import jax
import jax.numpy as jnp
from jax import lax
from jax.experimental import pallas as pl
from jax.experimental.pallas import tpu as pltpu
from jax.sharding import PartitionSpec as P

CAP = 64
DIRS = 8
GAMMA = (8.0 / 15.0, 5.0 / 12.0, 3.0 / 4.0)
ZETA = (0.0, -17.0 / 60.0, -5.0 / 12.0)
SENT_XP = (0, 4, 6)
SENT_XM = (1, 5, 7)
FROM_XP = (1, None, None)
FROM_XM = (0, None, None)
FROM_YP = (3, 5, 6)
FROM_YM = (2, 7, 4)
SPARE = 8
VMEM_BYTES = 16 * 2**20


def shifted(x, axis, by):
    size = lax.axis_size(axis)
    return lax.ppermute(x, axis, [(i, (i + by) % size) for i in range(size)])


def scatter_rows(state_ref, arrivals, target_ref):
    for ref, dirs in zip(arrivals, (FROM_XP, FROM_XM, FROM_YP, FROM_YM)):
        for place, d in enumerate(dirs):
            if d is None:
                continue

            def body(t, carry, ref=ref, place=place, d=d):
                slot = target_ref[d * CAP + t]
                state_ref[pl.ds(slot, 1), :] = ref[pl.ds(place * CAP + t, 1), :]
                return carry

            lax.fori_loop(0, CAP, body, 0, unroll=16)


def pack_rows(state_ref, out_ref, dirs, order_ref):
    for place, d in enumerate(dirs):

        def body(t, carry, place=place, d=d):
            slot = order_ref[d * CAP + t]
            out_ref[pl.ds(place * CAP + t, 1), :] = state_ref[pl.ds(slot, 1), :]
            return carry

        lax.fori_loop(0, CAP, body, 0, unroll=16)


def hat(base, frac, length):
    steps = lax.broadcasted_iota(jnp.int32, (length, base.shape[1]), 0) - base
    return jnp.where(steps == 0, 1.0 - frac, jnp.where(steps == 1, frac, 0.0))


def advance(section, first, lanes, *refs):
    if first:
        order_ref, cells_ref, inner_ref, rim_ref, source_ref, state_ref = refs[:6]
        outs = refs[6:]
    else:
        order_ref, target_ref, cells_ref, inner_ref, rim_ref, source_ref = refs[:6]
        arrivals = refs[6:10]
        state_ref = refs[10]
        outs = refs[11:]
        state_ref[...] = source_ref[...]
        scatter_rows(state_ref, arrivals, target_ref)
        source_ref = state_ref
    count = cells_ref.shape[1]
    width_x, width_y, depth = inner_ref.shape[1:]
    planes = []
    for k in range(3):
        inner = inner_ref[k].reshape(width_x * width_y, depth)
        planes.append(jnp.concatenate([inner.T, rim_ref[k].T], axis=1))
    plane = jnp.concatenate(planes, axis=0)
    rim = rim_ref.shape[1]
    pad = rim - 2 * (width_x + width_y) - 4
    for start in range(0, count, lanes):
        rows = source_ref[start : start + lanes, :]
        turned = rows.T
        frac = turned[0:3]
        before = turned[3:6]
        cell = cells_ref[:, start : start + lanes]
        cx, cy, cz = cell[0:1], cell[1:2], cell[2:3]
        fx, fy, fz = frac[0:1], frac[1:2], frac[2:3]
        wx = hat(cx, fx, width_x)
        wy = hat(cy, fy, width_y)
        wz = hat(cz, fz, depth)
        x_low = jnp.where(cx == -1, 1.0 - fx, 0.0)
        x_high = jnp.where(cx == width_x - 1, fx, 0.0)
        y_low = jnp.where(cy == -1, 1.0 - fy, 0.0)
        y_high = jnp.where(cy == width_y - 1, fy, 0.0)
        inner = (wx[:, None, :] * wy[None, :, :]).reshape(width_x * width_y, lanes)
        corners = [x_low * y_low, x_low * y_high, x_high * y_low, x_high * y_high]
        weight = jnp.concatenate(
            [inner, x_low * wy, x_high * wy, y_low * wx, y_high * wx, *corners, jnp.zeros((pad, lanes), jnp.float32)],
            axis=0,
        )
        high = weight.astype(jnp.bfloat16)
        low = (weight - high.astype(jnp.float32)).astype(jnp.bfloat16)
        columns = jnp.dot(plane, high, preferred_element_type=jnp.float32) + jnp.dot(
            plane, low, preferred_element_type=jnp.float32
        )
        speed = [
            jnp.sum(columns[k * depth : (k + 1) * depth] * wz, axis=0, keepdims=True) for k in range(3)
        ]
        speed = jnp.concatenate(speed, axis=0)
        moved = frac + GAMMA[section] * speed + ZETA[section] * before
        fresh = jnp.concatenate([moved, speed, jnp.zeros((2, lanes), jnp.float32)], axis=0).T
        if first:
            state_ref[start : start + lanes, :] = rows
        state_ref[start : start + lanes, 0:6] = fresh[:, 0:6]
    for out_ref, dirs in zip(outs, (SENT_XP, SENT_XM, (2,), (3,))):
        pack_rows(state_ref, out_ref, dirs, order_ref)


def finish(target_ref, state_ref, a_ref, b_ref, c_ref, d_ref, out_ref, work_ref):
    count = out_ref.shape[0]
    work_ref[...] = state_ref[...]
    scatter_rows(work_ref, (a_ref, b_ref, c_ref, d_ref), target_ref)
    out_ref[...] = work_ref[0:count, :]


def local(state, velocity, cells, slots, counts):
    sections = velocity.shape[0]
    width_x, width_y, depth = velocity.shape[2:]
    count, columns = state.shape
    vmem = pl.BlockSpec(memory_space=pltpu.VMEM)
    smem = pl.BlockSpec(memory_space=pltpu.SMEM)

    low_x = shifted(velocity[:, :, width_x - 1], "gx", 1)
    high_x = shifted(velocity[:, :, 0], "gx", -1)
    rows = jnp.concatenate(
        [velocity[:, :, :, width_y - 1], low_x[:, :, width_y - 1 :], high_x[:, :, width_y - 1 :]], axis=2
    )
    low_y = shifted(rows, "gy", 1)
    rows = jnp.concatenate([velocity[:, :, :, 0], low_x[:, :, :1], high_x[:, :, :1]], axis=2)
    high_y = shifted(rows, "gy", -1)
    corners = [
        low_y[:, :, width_x : width_x + 1],
        high_y[:, :, width_x : width_x + 1],
        low_y[:, :, width_x + 1 :],
        high_y[:, :, width_x + 1 :],
    ]
    rim = [low_x, high_x, low_y[:, :, :width_x], high_y[:, :, :width_x], *corners]
    used = 2 * (width_x + width_y) + 4
    pad = -used % 16
    rim = jnp.concatenate([*rim, jnp.zeros((sections, 3, pad, depth), velocity.dtype)], axis=2)

    within = jnp.arange(CAP, dtype=jnp.int32)
    order = slots[:, : DIRS * CAP]
    taken = within[None, None, :] < counts.reshape(sections, DIRS)[:, :, None]
    targets = jnp.where(taken.reshape(sections, DIRS * CAP), order, count)

    lanes = 256
    shapes = [
        jax.ShapeDtypeStruct((count + SPARE, columns), jnp.float32),
        jax.ShapeDtypeStruct((3 * CAP, columns), jnp.float32),
        jax.ShapeDtypeStruct((3 * CAP, columns), jnp.float32),
        jax.ShapeDtypeStruct((CAP, columns), jnp.float32),
        jax.ShapeDtypeStruct((CAP, columns), jnp.float32),
    ]
    arrivals = None
    for section in range(sections):
        first = section == 0
        operands = [order[section]] + ([] if first else [targets[section - 1]])
        specs = [smem] * len(operands)
        operands += [cells[section], velocity[section], rim[section], state]
        specs += [vmem] * 4
        if not first:
            operands += arrivals
            specs += [vmem] * 4
        state, xp, xm, yp, ym = pl.pallas_call(
            functools.partial(advance, section, first, lanes),
            out_shape=shapes,
            in_specs=specs,
            out_specs=[vmem] * 5,
            compiler_params=pltpu.CompilerParams(vmem_limit_bytes=VMEM_BYTES),
            name=f"advance{section}",
        )(*operands)
        from_low_x = shifted(xp, "gx", 1)
        from_high_x = shifted(xm, "gx", -1)
        from_low_y = shifted(
            jnp.concatenate([yp, from_low_x[CAP : 2 * CAP], from_high_x[2 * CAP :]], axis=0), "gy", 1
        )
        from_high_y = shifted(
            jnp.concatenate([ym, from_low_x[2 * CAP :], from_high_x[CAP : 2 * CAP]], axis=0), "gy", -1
        )
        arrivals = [from_low_x, from_high_x, from_low_y, from_high_y]
    return pl.pallas_call(
        finish,
        out_shape=jax.ShapeDtypeStruct((count, columns), jnp.float32),
        in_specs=[smem] + [vmem] * 5,
        out_specs=vmem,
        scratch_shapes=[pltpu.VMEM((count + SPARE, columns), jnp.float32)],
        compiler_params=pltpu.CompilerParams(vmem_limit_bytes=VMEM_BYTES),
        name="finish",
    )(targets[sections - 1], state, *arrivals)


def solution(mesh):
    return jax.shard_map(
        local,
        mesh=mesh,
        in_specs=(
            P(("gx", "gy"), None),
            P(None, None, "gx", "gy", None),
            P(None, None, ("gx", "gy")),
            P(None, ("gx", "gy")),
            P(None, "gx", "gy", None),
        ),
        out_specs=P(("gx", "gy"), None),
        check_vma=False,
    )
```

```python
import functools

import jax
import jax.numpy as jnp
from jax import lax
from jax.experimental import pallas as pl
from jax.experimental.pallas import tpu as pltpu
from jax.sharding import PartitionSpec as P


CAP = 64
DIRS = 8
GAMMA = (8.0 / 15.0, 5.0 / 12.0, 3.0 / 4.0)
ZETA = (0.0, -17.0 / 60.0, -5.0 / 12.0)
SEGMENTS = (0, 4, 6, 1, 5, 7, 2, 3)
FROM_XP = (1, None, None)
FROM_XM = (0, None, None)
FROM_YP = (3, 5, 6)
FROM_YM = (2, 7, 4)
SPARE = 8
UNROLL = 16
VMEM_BYTES = 16 * 2**20
LANES = 256


def shifted(x, axis, by):
    size = lax.axis_size(axis)
    return lax.ppermute(x, axis, [(i, (i + by) % size) for i in range(size)])


def scatter_rows(state_ref, target_ref, arrivals):
    for ref, dirs in arrivals:
        for place, d in enumerate(dirs):
            if d is None:
                continue

            def body(t, carry, ref=ref, place=place, d=d):
                slot = target_ref[d * CAP + t]
                state_ref[pl.ds(slot, 1), :] = ref[pl.ds(place * CAP + t, 1), :]
                return carry

            lax.fori_loop(0, CAP, body, 0, unroll=UNROLL)


def gather_rows(slot_ref, *pairs):
    def body(t, carry):
        slot = slot_ref[t]
        for out_ref, from_ref in pairs:
            out_ref[pl.ds(t, 1), :] = from_ref[pl.ds(slot, 1), :]
        return carry

    lax.fori_loop(0, slot_ref.shape[0], body, 0, unroll=UNROLL)


def hat(base, frac, length):
    steps = lax.broadcasted_iota(jnp.int32, (length, base.shape[1]), 0) - base
    return jnp.where(steps == 0, 1.0 - frac, jnp.where(steps == 1, frac, 0.0))


def split_wide(value):
    high = value.astype(jnp.bfloat16)
    return high, value - high.astype(jnp.float32)


def split(weight):
    high = weight.astype(jnp.bfloat16)
    return high, (weight - high.astype(jnp.float32)).astype(jnp.bfloat16)


def advanced(section, turned, cell, plane, rim, widths):
    width_x, width_y, depth = widths
    lanes = cell.shape[1]
    frac, before = turned[0:3], turned[3:6]
    cx, cy, cz = cell[0:1], cell[1:2], cell[2:3]
    fx, fy, fz = frac[0:1], frac[1:2], frac[2:3]
    wx = hat(cx, fx, width_x)
    wy = hat(cy, fy, width_y)
    wz = hat(cz, fz, depth)
    x_low = jnp.where(cx == -1, 1.0 - fx, 0.0)
    x_high = jnp.where(cx == width_x - 1, fx, 0.0)
    y_low = jnp.where(cy == -1, 1.0 - fy, 0.0)
    y_high = jnp.where(cy == width_y - 1, fy, 0.0)
    inner = (wx[:, None, :] * wy[None, :, :]).reshape(width_x * width_y, lanes)
    corners = [x_low * y_low, x_high * y_low, x_low * y_high, x_high * y_high]
    pad = rim.shape[1] // 2 - 2 * (width_x + width_y) - 4
    edge = jnp.concatenate(
        [x_low * wy, x_high * wy, y_low * wx, y_high * wx, *corners, jnp.zeros((pad, lanes), jnp.float32)], axis=0
    )
    high, low = split(inner)
    columns = jnp.dot(plane, high, preferred_element_type=jnp.float32)
    columns += jnp.dot(plane, low, preferred_element_type=jnp.float32)
    columns += jnp.dot(rim, jnp.concatenate(split(edge), axis=0), preferred_element_type=jnp.float32)
    speed = jnp.concatenate(
        [jnp.sum(columns[k * depth : (k + 1) * depth] * wz, axis=0, keepdims=True) for k in range(3)], axis=0
    )
    moved = frac + GAMMA[section] * speed + ZETA[section] * before
    return jnp.concatenate([moved, speed, jnp.zeros((2, lanes), jnp.float32)], axis=0)


def turn_rim(section, halo, out_ref):
    low_x, high_x, low_y, high_y = halo
    width_x, width_y, depth = low_y.shape[2] - 2, low_x.shape[2], low_x.shape[3]
    pad = out_ref.shape[1] // 2 - 2 * (width_x + width_y)
    spot = lax.broadcasted_iota(jnp.int32, (pad, depth), 0)
    for k in range(3):
        corners = jnp.zeros((pad, depth), jnp.float32)
        for n, (ref, row) in enumerate(
            ((low_y, width_x), (low_y, width_x + 1), (high_y, width_x), (high_y, width_x + 1))
        ):
            value = ref[section, k, row : row + 1, :].astype(jnp.float32)
            corners = jnp.where(spot == n, value, corners)
        rim = jnp.concatenate(
            [
                low_x[section, k],
                high_x[section, k],
                low_y[section, k, 0:width_x, :],
                high_y[section, k, 0:width_x, :],
                corners.astype(out_ref.dtype),
            ],
            axis=0,
        )
        turned = rim.T
        out_ref[k * depth : (k + 1) * depth, :] = jnp.concatenate([turned, turned], axis=1)


def turn_plane(velocity_ref, section, out_ref):
    width_x, width_y, depth = velocity_ref.shape[2:]
    for k in range(3):
        plane = velocity_ref[section, k].reshape(width_x * width_y, depth)
        out_ref[k * depth : (k + 1) * depth, :] = plane.T


def fetch(*refs):
    sources, (state_ref, velocity_ref, cells_ref) = refs[:5], refs[5:8]
    low_ref, high_ref, plane_ref, rows_ref, leave_ref, arrive_ref, target_ref = refs[8:15]
    slots_ref, counts_ref, sems = refs[15:]
    copies = [
        pltpu.make_async_copy(src, dst, sems.at[n])
        for n, (src, dst) in enumerate(
            zip(sources, (velocity_ref, slots_ref, counts_ref, cells_ref, state_ref))
        )
    ]
    for copy in copies:
        copy.start()
    sections, parts, count = cells_ref.shape
    width_y = velocity_ref.shape[3]
    leaving = leave_ref.shape[2]

    copies[1].wait()
    copies[2].wait()
    place = lax.broadcasted_iota(jnp.int32, (DIRS, leaving), 1)
    start = lax.broadcasted_iota(jnp.int32, (DIRS, leaving), 0) * CAP
    spread = jnp.where((place >= start) & (place < start + CAP), 1.0, 0.0)
    tally = jnp.concatenate(
        [counts_ref[s, 0].astype(jnp.float32) for s in range(sections)]
        + [jnp.zeros((-sections % 8, DIRS), jnp.float32)],
        axis=0,
    )
    limit = jnp.dot(tally, spread, preferred_element_type=jnp.float32).astype(jnp.int32)
    within = lax.broadcasted_iota(jnp.int32, (1, leaving), 1) % CAP
    for s in range(sections):
        order = slots_ref[s : s + 1, 0:leaving]
        target = jnp.where(within < limit[s : s + 1], order, count)
        target_ref[s] = target
        leave_ref[s] = jnp.concatenate([order[:, d * CAP : (d + 1) * CAP] for d in SEGMENTS], axis=1)
        arrive_ref[s] = jnp.concatenate(
            [target[:, d * CAP : (d + 1) * CAP] for d in FROM_YP + FROM_YM], axis=1
        )
    copies[0].wait()
    for s in range(sections):
        for k in range(3):
            block = velocity_ref[s, k].astype(jnp.float32)
            low_ref[s, k] = block[:, 0, :].astype(low_ref.dtype)
            high_ref[s, k] = block[:, width_y - 1, :].astype(low_ref.dtype)
    turn_plane(velocity_ref, 0, plane_ref)
    copies[3].wait()
    flat = jnp.concatenate(
        [cells_ref[s].astype(jnp.float32) for s in range(sections)]
        + [jnp.zeros((-sections * parts % 8, count), jnp.float32)],
        axis=0,
    )
    rows_ref[:, 0 : flat.shape[0]] = flat.T
    copies[4].wait()


def own_cells(section, part_ref, cell_ref):
    parts = cell_ref.shape[0]
    cell_ref[...] = part_ref[...].T[section * parts : (section + 1) * parts].astype(jnp.int32)


def first(slot_ref, rows_ref, state_ref, left_ref, cell_ref, part_ref):
    gather_rows(slot_ref, (left_ref, state_ref), (part_ref, rows_ref))
    own_cells(0, part_ref, cell_ref)


def depart(section, widths, *refs):
    left_ref, cell_ref, plane_ref = refs[:3]
    leaving = left_ref.shape[0]
    if section == 0:
        halo, turned_ref, outs = refs[3:7], refs[7], refs[8:]
        turn_rim(section, halo, turned_ref)
        rows = left_ref[...]
    else:
        turned_ref, pick_ref, c_ref, d_ref = refs[3:7]
        outs = refs[7:]
        arrived = jnp.concatenate([c_ref[...], d_ref[...]], axis=0)
        high, rest = split_wide(arrived)
        middle, low = split(rest)
        rows = left_ref[...]
        for part in (high, middle, low):
            rows += jnp.dot(pick_ref[...], part, preferred_element_type=jnp.float32)
    fresh = []
    for start in range(0, leaving, LANES):
        stop = start + LANES
        cell = cell_ref[:, start:stop]
        new = advanced(section, rows[start:stop].T, cell, plane_ref[...], turned_ref[...], widths)
        fresh.append(new.T[:, 0:6])
    start = 0
    for ref in outs:
        stop = start + ref.shape[0]
        ref[...] = rows[start:stop]
        for n, part in enumerate(fresh):
            low, high = max(start, n * LANES), min(stop, (n + 1) * LANES)
            if low < high:
                ref[low - start : high - start, 0:6] = part[low - n * LANES : high - n * LANES]
        start = stop


def advance(section, widths, more, *refs):
    if section:
        target_ref, c_ref, d_ref, *refs = refs
    cells_ref, plane_ref, turned_ref, state_ref, *refs = refs
    if more:
        velocity_ref, *halo, out_ref, next_plane_ref, next_ref = refs
    else:
        (out_ref,) = refs
    if section:
        out_ref[...] = state_ref[...]
        scatter_rows(out_ref, target_ref, ((c_ref, FROM_YP), (d_ref, FROM_YM)))
        state_ref = out_ref
    count = cells_ref.shape[2]
    for start in range(0, count, LANES):
        rows = state_ref[start : start + LANES, :]
        cell = cells_ref[section, :, start : start + LANES]
        new = advanced(section, rows.T, cell, plane_ref[...], turned_ref[...], widths)
        if section == 0:
            out_ref[start : start + LANES, :] = rows
        out_ref[start : start + LANES, 0:6] = new.T[:, 0:6]
    if more:
        turn_plane(velocity_ref, section + 1, next_plane_ref)
        turn_rim(section + 1, halo, next_ref)


def settle(section, more, target_ref, *refs):
    if more:
        slot_ref, old_ref, a_ref, b_ref, rows_ref, leave_ref, arrive_ref = refs[:7]
        state_ref, left_ref, cell_ref, pick_ref, part_ref = refs[7:]
    else:
        old_ref, a_ref, b_ref, state_ref = refs
    state_ref[0 : old_ref.shape[0], :] = old_ref[...]
    scatter_rows(state_ref, target_ref, ((a_ref, FROM_XP), (b_ref, FROM_XM)))
    if more:
        leaving = left_ref.shape[0]
        gather_rows(slot_ref, (left_ref, state_ref), (part_ref, rows_ref))
        own_cells(section + 1, part_ref, cell_ref)
        leave = jnp.broadcast_to(leave_ref[section + 1].astype(jnp.float32), (8, leaving)).T[:, 0:1]
        pick = jnp.where(leave == arrive_ref[section].astype(jnp.float32), 1.0, 0.0)
        pick_ref[...] = pick.astype(pick_ref.dtype)
        left_ref[...] = jnp.where(jnp.max(pick, axis=1, keepdims=True) > 0.0, 0.0, left_ref[...])


def finish(target_ref, old_ref, c_ref, d_ref, out_ref, work_ref):
    count = out_ref.shape[0]
    work_ref[...] = old_ref[...]
    scatter_rows(work_ref, target_ref, ((c_ref, FROM_YP), (d_ref, FROM_YM)))
    out_ref[...] = work_ref[0:count, :]


def local(state, velocity, cells, slots, counts):
    sections = velocity.shape[0]
    width_x, width_y, depth = widths = velocity.shape[2:]
    count, columns = state.shape
    leaving = DIRS * CAP
    coming = CAP * (len(FROM_YP) + len(FROM_YM))
    vmem = pl.BlockSpec(memory_space=pltpu.VMEM)
    smem = pl.BlockSpec(memory_space=pltpu.SMEM)
    hbm = pl.BlockSpec(memory_space=pltpu.HBM)
    params = pltpu.CompilerParams(vmem_limit_bytes=VMEM_BYTES)

    def shape(*dims, dtype=jnp.float32):
        return jax.ShapeDtypeStruct(dims, dtype)

    def call(body, operands, scalars, outs, scratch=(), specs=None):
        single = len(outs) == 1
        return pl.pallas_call(
            body,
            out_shape=outs[0] if single else outs,
            in_specs=specs or [smem] * scalars + [vmem] * (len(operands) - scalars),
            out_specs=vmem if single else [vmem] * len(outs),
            scratch_shapes=scratch,
            compiler_params=params,
        )(*operands)

    plane_shape = shape(3 * depth, width_x * width_y, dtype=velocity.dtype)
    edge_shape = shape(sections, 3, width_x, depth, dtype=velocity.dtype)
    cell_shape = shape(3, leaving, dtype=jnp.int32)
    gathered = pltpu.VMEM((leaving, columns), jnp.float32)

    low_x = shifted(velocity[:, :, width_x - 1], "gx", 1)
    high_x = shifted(velocity[:, :, 0], "gx", -1)
    sources = (velocity, slots, counts, cells, state)
    state, velocity, cells, bottom, top, plane, rows, leave, arrive, target = call(
        fetch,
        [pltpu.with_memory_space_constraint(x, pltpu.HBM) for x in sources],
        0,
        [
            shape(*state.shape),
            shape(*velocity.shape, dtype=velocity.dtype),
            shape(*cells.shape, dtype=cells.dtype),
            edge_shape,
            edge_shape,
            plane_shape,
            shape(count, columns),
            shape(sections, 1, leaving, dtype=jnp.int32),
            shape(sections, 1, coming, dtype=jnp.int32),
            shape(sections, 1, leaving, dtype=jnp.int32),
        ],
        [
            pltpu.VMEM(slots.shape, slots.dtype),
            pltpu.VMEM(counts.shape, counts.dtype),
            pltpu.SemaphoreType.DMA((5,)),
        ],
        [hbm] * 5,
    )
    low_y = shifted(
        jnp.concatenate([top, low_x[:, :, width_y - 1 :], high_x[:, :, width_y - 1 :]], axis=2),
        "gy",
        1,
    )
    high_y = shifted(jnp.concatenate([bottom, low_x[:, :, :1], high_x[:, :, :1]], axis=2), "gy", -1)
    halo = [low_x, high_x, low_y, high_y]
    used = 2 * (width_x + width_y) + 4
    turned_shape = shape(3 * depth, 2 * (used + -used % 16), dtype=velocity.dtype)
    targets = [target[section].reshape(leaving) for section in range(sections)]
    slot = [leave[section].reshape(leaving) for section in range(sections)]

    left, cell = call(
        first, [slot[0], rows, state], 1, [shape(leaving, columns), cell_shape], [gathered]
    )
    messages = [shape(3 * CAP, columns)] * 2 + [shape(CAP, columns)] * 2
    for section in range(sections):
        more = section + 1 < sections
        body = functools.partial(depart, section, widths)
        if section == 0:
            turned, *sent = call(body, [left, cell, plane, *halo], 0, [turned_shape, *messages])
        else:
            sent = call(
                body, [left, cell, plane, turned, pick, from_low_y, from_high_y], 0, messages
            )
        xp, xm, yp, ym = sent
        from_low_x = shifted(xp, "gx", 1)
        from_high_x = shifted(xm, "gx", -1)
        out = call(
            functools.partial(advance, section, widths, more),
            ([targets[section - 1], from_low_y, from_high_y] if section else [])
            + [cells, plane, turned, state]
            + ([velocity, *halo] if more else []),
            1 if section else 0,
            [shape(count + SPARE if section else count, columns)]
            + ([plane_shape, turned_shape] if more else []),
        )
        state, plane, turned = out if more else (out, None, None)
        from_low_y = shifted(
            jnp.concatenate([yp, from_low_x[CAP : 2 * CAP], from_high_x[2 * CAP :]], axis=0),
            "gy",
            1,
        )
        from_high_y = shifted(
            jnp.concatenate([ym, from_low_x[2 * CAP :], from_high_x[CAP : 2 * CAP]], axis=0),
            "gy",
            -1,
        )
        out = call(
            functools.partial(settle, section, more),
            [targets[section]]
            + ([slot[section + 1]] if more else [])
            + [state, from_low_x, from_high_x]
            + ([rows, leave, arrive] if more else []),
            2 if more else 1,
            [shape(count + SPARE, columns)]
            + (
                [shape(leaving, columns), cell_shape, shape(leaving, coming, dtype=jnp.bfloat16)]
                if more
                else []
            ),
            [gathered] if more else [],
        )
        state, left, cell, pick = out if more else (out, None, None, None)
    return call(
        finish,
        [targets[sections - 1], state, from_low_y, from_high_y],
        1,
        [shape(count, columns)],
        [pltpu.VMEM((count + SPARE, columns), jnp.float32)],
    )


def solution(mesh):
    return jax.shard_map(
        local,
        mesh=mesh,
        in_specs=(
            P(("gx", "gy"), None),
            P(None, None, "gx", "gy", None),
            P(None, None, ("gx", "gy")),
            P(None, ("gx", "gy")),
            P(None, "gx", "gy", None),
        ),
        out_specs=P(("gx", "gy"), None),
        check_vma=False,
    )
```

```python
import functools

import jax
import jax.numpy as jnp
from jax import lax
from jax.experimental import pallas as pl
from jax.experimental.pallas import tpu as pltpu
from jax.sharding import PartitionSpec as P


CAP = 64
DIRS = 8
GAMMA = (8.0 / 15.0, 5.0 / 12.0, 3.0 / 4.0)
ZETA = (0.0, -17.0 / 60.0, -5.0 / 12.0)
SEGMENTS = (0, 4, 6, 1, 5, 7, 2, 3)
FROM_XP = (1, None, None)
FROM_XM = (0, None, None)
FROM_YP = (3, 5, 6)
FROM_YM = (2, 7, 4)
TAIL = 8
SEGMENT = CAP + TAIL
RANGE = 2.0**15
SHRINK = 2.0**-10
SECOND = 2.0**11
TINY = 2.0**-14
NUDGE = 0.75 * 2.0**-12
SPARE = 8
UNROLL = 16
VMEM_BYTES = 16 * 2**20
LANES = 256
PIECES = 1


def shifted(x, axis, by):
    size = lax.axis_size(axis)
    return lax.ppermute(x, axis, [(i, (i + by) % size) for i in range(size)])


def scatter_rows(state_ref, target_ref, arrivals):
    for ref, dirs in arrivals:
        for place, d in enumerate(dirs):
            if d is None:
                continue

            def body(t, carry, ref=ref, place=place, d=d):
                slot = target_ref[d * CAP + t]
                state_ref[pl.ds(slot, 1), :] = ref[pl.ds(place * CAP + t, 1), :]
                return carry

            lax.fori_loop(0, CAP, body, 0, unroll=UNROLL)


def gather_rows(slot_ref, *pairs):
    def body(t, carry):
        slot = slot_ref[t]
        for out_ref, from_ref in pairs:
            out_ref[pl.ds(t, 1), :] = from_ref[pl.ds(slot, 1), :]
        return carry

    lax.fori_loop(0, slot_ref.shape[0], body, 0, unroll=UNROLL)


def hat(base, frac, length):
    steps = lax.broadcasted_iota(jnp.int32, (length, base.shape[1]), 0) - base
    return jnp.where(steps == 0, 1.0 - frac, jnp.where(steps == 1, frac, 0.0))


def eleven_bits(value):
    wide = value * 8193.0
    return wide - (wide - value)


def encoded(rows):
    value = rows * RANGE
    code = eleven_bits(value)
    return jnp.where(value >= code, code, -code)


def encoded_first(columns):
    value = columns * SHRINK
    high = jnp.where(jnp.abs(value) < TINY, (value + 0.75) - 0.75, eleven_bits(value))
    return high, (value - high) * SECOND


def decode(message_ref, place, out_ref, out_place):
    start, stop = place * SEGMENT, place * SEGMENT + CAP
    code = message_ref[start:stop, :]
    second = message_ref[stop : stop + TAIL, :].T[0:CAP, 0:6]
    rows = pl.ds(out_place * CAP, CAP)
    out_ref[rows, :] = jnp.abs(code) * jnp.where(code < 0.0, (1.0 - NUDGE) / RANGE, (1.0 + NUDGE) / RANGE)
    out_ref[rows, 0:6] = (code[:, 0:6] + second * (1.0 / SECOND)) * (1.0 / SHRINK)


def split_wide(value):
    high = value.astype(jnp.bfloat16)
    return high, value - high.astype(jnp.float32)


def split(weight):
    high = weight.astype(jnp.bfloat16)
    return high, (weight - high.astype(jnp.float32)).astype(jnp.bfloat16)


def advanced(section, turned, cell, plane, rim, widths):
    width_x, width_y, depth = widths
    lanes = cell.shape[1]
    frac, before = turned[0:3], turned[3:6]
    cx, cy, cz = cell[0:1], cell[1:2], cell[2:3]
    fx, fy, fz = frac[0:1], frac[1:2], frac[2:3]
    wx = hat(cx, fx, width_x)
    wy = hat(cy, fy, width_y)
    wz = hat(cz, fz, depth)
    x_low = jnp.where(cx == -1, 1.0 - fx, 0.0)
    x_high = jnp.where(cx == width_x - 1, fx, 0.0)
    y_low = jnp.where(cy == -1, 1.0 - fy, 0.0)
    y_high = jnp.where(cy == width_y - 1, fy, 0.0)
    inner = (wx[:, None, :] * wy[None, :, :]).reshape(width_x * width_y, lanes)
    corners = [x_low * y_low, x_high * y_low, x_low * y_high, x_high * y_high]
    pad = rim.shape[1] // 2 - 2 * (width_x + width_y) - 4
    edge = jnp.concatenate(
        [x_low * wy, x_high * wy, y_low * wx, y_high * wx, *corners, jnp.zeros((pad, lanes), jnp.float32)], axis=0
    )
    high, low = split(inner)
    columns = jnp.dot(plane, high, preferred_element_type=jnp.float32)
    columns += jnp.dot(plane, low, preferred_element_type=jnp.float32)
    columns += jnp.dot(rim, jnp.concatenate(split(edge), axis=0), preferred_element_type=jnp.float32)
    speed = jnp.concatenate(
        [jnp.sum(columns[k * depth : (k + 1) * depth] * wz, axis=0, keepdims=True) for k in range(3)], axis=0
    )
    moved = frac + GAMMA[section] * speed + ZETA[section] * before
    return jnp.concatenate([moved, speed, jnp.zeros((2, lanes), jnp.float32)], axis=0)


def turn_rim(section, halo, out_ref):
    low_x, high_x, low_y, high_y = halo
    width_x, width_y, depth = low_y.shape[2] - 2, low_x.shape[2], low_x.shape[3]
    pad = out_ref.shape[1] // 2 - 2 * (width_x + width_y)
    spot = lax.broadcasted_iota(jnp.int32, (pad, depth), 0)
    for k in range(3):
        corners = jnp.zeros((pad, depth), jnp.float32)
        for n, (ref, row) in enumerate(
            ((low_y, width_x), (low_y, width_x + 1), (high_y, width_x), (high_y, width_x + 1))
        ):
            value = ref[section, k, row : row + 1, :].astype(jnp.float32)
            corners = jnp.where(spot == n, value, corners)
        rim = jnp.concatenate(
            [
                low_x[section, k],
                high_x[section, k],
                low_y[section, k, 0:width_x, :],
                high_y[section, k, 0:width_x, :],
                corners.astype(out_ref.dtype),
            ],
            axis=0,
        )
        turned = rim.T
        out_ref[k * depth : (k + 1) * depth, :] = jnp.concatenate([turned, turned], axis=1)


def turn_plane(velocity_ref, section, out_ref):
    width_x, width_y, depth = velocity_ref.shape[2:]
    for k in range(3):
        plane = velocity_ref[section, k].reshape(width_x * width_y, depth)
        out_ref[k * depth : (k + 1) * depth, :] = plane.T


def fetch(*refs):
    sources, (state_ref, velocity_ref, cells_ref) = refs[:5], refs[5:8]
    low_ref, high_ref, plane_ref, rows_ref, leave_ref, arrive_ref, target_ref = refs[8:15]
    slots_ref, counts_ref, sems = refs[15:]
    copies = [
        pltpu.make_async_copy(src, dst, sems.at[n])
        for n, (src, dst) in enumerate(
            zip(sources, (velocity_ref, slots_ref, counts_ref, cells_ref, state_ref))
        )
    ]
    for copy in copies:
        copy.start()
    sections, parts, count = cells_ref.shape
    width_y = velocity_ref.shape[3]
    leaving = leave_ref.shape[2]

    copies[1].wait()
    copies[2].wait()
    place = lax.broadcasted_iota(jnp.int32, (DIRS, leaving), 1)
    start = lax.broadcasted_iota(jnp.int32, (DIRS, leaving), 0) * CAP
    spread = jnp.where((place >= start) & (place < start + CAP), 1.0, 0.0)
    tally = jnp.concatenate(
        [counts_ref[s, 0].astype(jnp.float32) for s in range(sections)]
        + [jnp.zeros((-sections % 8, DIRS), jnp.float32)],
        axis=0,
    )
    limit = jnp.dot(tally, spread, preferred_element_type=jnp.float32).astype(jnp.int32)
    within = lax.broadcasted_iota(jnp.int32, (1, leaving), 1) % CAP
    for s in range(sections):
        order = slots_ref[s : s + 1, 0:leaving]
        target = jnp.where(within < limit[s : s + 1], order, count)
        target_ref[s] = target
        leave_ref[s] = jnp.concatenate([order[:, d * CAP : (d + 1) * CAP] for d in SEGMENTS], axis=1)
        arrive_ref[s] = jnp.concatenate(
            [target[:, d * CAP : (d + 1) * CAP] for d in FROM_YP + FROM_YM], axis=1
        )
    copies[0].wait()
    for s in range(sections):
        for k in range(3):
            block = velocity_ref[s, k].astype(jnp.float32)
            low_ref[s, k] = block[:, 0, :].astype(low_ref.dtype)
            high_ref[s, k] = block[:, width_y - 1, :].astype(low_ref.dtype)
    turn_plane(velocity_ref, 0, plane_ref)
    copies[3].wait()
    flat = jnp.concatenate(
        [cells_ref[s].astype(jnp.float32) for s in range(sections)]
        + [jnp.zeros((-sections * parts % 8, count), jnp.float32)],
        axis=0,
    )
    rows_ref[:, 0 : flat.shape[0]] = flat.T
    copies[4].wait()


def own_cells(section, part_ref, cell_ref):
    parts = cell_ref.shape[0]
    cell_ref[...] = part_ref[...].T[section * parts : (section + 1) * parts].astype(jnp.int32)


def first(slot_ref, rows_ref, state_ref, left_ref, cell_ref, part_ref):
    gather_rows(slot_ref, (left_ref, state_ref), (part_ref, rows_ref))
    own_cells(0, part_ref, cell_ref)


def depart(section, widths, *refs):
    left_ref, cell_ref, plane_ref = refs[:3]
    leaving = left_ref.shape[0]
    if section == 0:
        halo, turned_ref, outs = refs[3:7], refs[7], refs[8:]
        turn_rim(section, halo, turned_ref)
        rows = left_ref[...]
    else:
        turned_ref, pick_ref, c_ref, d_ref = refs[3:7]
        landed_ref, *outs = refs[7:]
        for n, ref in enumerate((c_ref, d_ref)):
            for place in range(3):
                decode(ref, place, landed_ref, 3 * n + place)
        arrived = landed_ref[...]
        high, rest = split_wide(arrived)
        middle, low = split(rest)
        columns = arrived.shape[1]
        put = jnp.dot(
            pick_ref[...],
            jnp.concatenate([high, middle, low], axis=1),
            preferred_element_type=jnp.float32,
        )
        rows = left_ref[...]
        for n in range(3):
            rows += put[:, n * columns : (n + 1) * columns]
    outs = [(ref, place) for ref in outs for place in range(ref.shape[0] // SEGMENT)]
    for start in range(0, leaving, LANES):
        cell = cell_ref[:, start : start + LANES]
        part = rows[start : start + LANES]
        new = advanced(section, part.T, cell, plane_ref[...], turned_ref[...], widths)
        high, low = encoded_first(new)
        code = encoded(part)
        turned = high.T
        for n in range(LANES // CAP):
            ref, place = outs[start // CAP + n]
            own = slice(n * CAP, (n + 1) * CAP)
            base = place * SEGMENT
            ref[base : base + CAP, :] = code[own]
            ref[base : base + CAP, 0:6] = turned[own, 0:6]
            ref[base + CAP : base + SEGMENT, :] = jnp.concatenate(
                [low[:, own], jnp.zeros((TAIL, ref.shape[1] - CAP), jnp.float32)], axis=1
            )


def advance(section, widths, more, *refs):
    if section:
        target_ref, landed_ref, *refs = refs
    cells_ref, plane_ref, turned_ref, state_ref, *refs = refs
    if more:
        velocity_ref, *halo, out_ref, next_plane_ref, next_ref = refs
    else:
        (out_ref,) = refs
    if section:
        out_ref[...] = state_ref[...]
        scatter_rows(out_ref, target_ref, ((landed_ref, FROM_YP + FROM_YM),))
        state_ref = out_ref
    count = cells_ref.shape[2]
    for start in range(0, count, LANES):
        rows = state_ref[start : start + LANES, :]
        cell = cells_ref[section, :, start : start + LANES]
        new = advanced(section, rows.T, cell, plane_ref[...], turned_ref[...], widths)
        if section == 0:
            out_ref[start : start + LANES, :] = rows
        out_ref[start : start + LANES, 0:6] = new.T[:, 0:6]
    if more:
        turn_plane(velocity_ref, section + 1, next_plane_ref)
        turn_rim(section + 1, halo, next_ref)


def settle(section, more, target_ref, *refs):
    if more:
        slot_ref, old_ref, a_ref, b_ref, rows_ref, leave_ref, arrive_ref = refs[:7]
        state_ref, left_ref, cell_ref, pick_ref, landed_ref, part_ref = refs[7:]
    else:
        old_ref, a_ref, b_ref, state_ref, landed_ref = refs
    decode(a_ref, 0, landed_ref, 0)
    decode(b_ref, 0, landed_ref, 1)
    state_ref[0 : old_ref.shape[0], :] = old_ref[...]
    scatter_rows(state_ref, target_ref, ((landed_ref, (FROM_XP[0], FROM_XM[0])),))
    if more:
        leaving = left_ref.shape[0]
        gather_rows(slot_ref, (left_ref, state_ref), (part_ref, rows_ref))
        own_cells(section + 1, part_ref, cell_ref)
        leave = jnp.broadcast_to(leave_ref[section + 1].astype(jnp.float32), (8, leaving)).T[:, 0:1]
        pick = jnp.where(leave == arrive_ref[section].astype(jnp.float32), 1.0, 0.0)
        pick_ref[...] = pick.astype(pick_ref.dtype)
        left_ref[...] = jnp.where(jnp.max(pick, axis=1, keepdims=True) > 0.0, 0.0, left_ref[...])


def land(target_ref, old_ref, c_ref, state_ref, landed_ref):
    state_ref[...] = old_ref[...]
    for place in range(3):
        decode(c_ref, place, landed_ref, place)
    scatter_rows(state_ref, target_ref, ((landed_ref, FROM_YP),))


def finish(target_ref, old_ref, d_ref, out_hbm, work_ref, landed_ref, sems):
    count = out_hbm.shape[0]
    work_ref[...] = old_ref[...]
    for place in range(3):
        decode(d_ref, place, landed_ref, place)
    scatter_rows(work_ref, target_ref, ((landed_ref, FROM_YM),))
    step = count // PIECES
    copies = [
        pltpu.make_async_copy(
            work_ref.at[pl.ds(n * step, step), :], out_hbm.at[pl.ds(n * step, step), :], sems.at[n]
        )
        for n in range(PIECES)
    ]
    for copy in copies:
        copy.start()
    for copy in copies:
        copy.wait()


def local(state, velocity, cells, slots, counts):
    sections = velocity.shape[0]
    width_x, width_y, depth = widths = velocity.shape[2:]
    count, columns = state.shape
    leaving = DIRS * CAP
    coming = CAP * (len(FROM_YP) + len(FROM_YM))
    vmem = pl.BlockSpec(memory_space=pltpu.VMEM)
    smem = pl.BlockSpec(memory_space=pltpu.SMEM)
    hbm = pl.BlockSpec(memory_space=pltpu.HBM)
    params = pltpu.CompilerParams(vmem_limit_bytes=VMEM_BYTES)

    def shape(*dims, dtype=jnp.float32):
        return jax.ShapeDtypeStruct(dims, dtype)

    def call(body, operands, scalars, outs, scratch=(), specs=None):
        single = len(outs) == 1
        return pl.pallas_call(
            body,
            out_shape=outs[0] if single else outs,
            in_specs=specs or [smem] * scalars + [vmem] * (len(operands) - scalars),
            out_specs=vmem if single else [vmem] * len(outs),
            scratch_shapes=scratch,
            compiler_params=params,
        )(*operands)

    plane_shape = shape(3 * depth, width_x * width_y, dtype=velocity.dtype)
    edge_shape = shape(sections, 3, width_x, depth, dtype=velocity.dtype)
    cell_shape = shape(3, leaving, dtype=jnp.int32)
    gathered = pltpu.VMEM((leaving, columns), jnp.float32)

    low_x = shifted(velocity[:, :, width_x - 1], "gx", 1)
    high_x = shifted(velocity[:, :, 0], "gx", -1)
    sources = (velocity, slots, counts, cells, state)
    state, velocity, cells, bottom, top, plane, rows, leave, arrive, target = call(
        fetch,
        [pltpu.with_memory_space_constraint(x, pltpu.HBM) for x in sources],
        0,
        [
            shape(*state.shape),
            shape(*velocity.shape, dtype=velocity.dtype),
            shape(*cells.shape, dtype=cells.dtype),
            edge_shape,
            edge_shape,
            plane_shape,
            shape(count, columns),
            shape(sections, 1, leaving, dtype=jnp.int32),
            shape(sections, 1, coming, dtype=jnp.int32),
            shape(sections, 1, leaving, dtype=jnp.int32),
        ],
        [
            pltpu.VMEM(slots.shape, slots.dtype),
            pltpu.VMEM(counts.shape, counts.dtype),
            pltpu.SemaphoreType.DMA((5,)),
        ],
        [hbm] * 5,
    )
    low_y = shifted(jnp.concatenate([top, low_x[:, :, width_y - 1 :], high_x[:, :, width_y - 1 :]], axis=2), "gy", 1)
    high_y = shifted(jnp.concatenate([bottom, low_x[:, :, :1], high_x[:, :, :1]], axis=2), "gy", -1)
    halo = [low_x, high_x, low_y, high_y]
    used = 2 * (width_x + width_y) + 4
    turned_shape = shape(3 * depth, 2 * (used + -used % 16), dtype=velocity.dtype)
    targets = [target[section].reshape(leaving) for section in range(sections)]
    slot = [leave[section].reshape(leaving) for section in range(sections)]

    left, cell = call(first, [slot[0], rows, state], 1, [shape(leaving, columns), cell_shape], [gathered])
    messages = [shape(3 * SEGMENT, columns)] * 2 + [shape(SEGMENT, columns)] * 2
    for section in range(sections):
        more = section + 1 < sections
        body = functools.partial(depart, section, widths)
        if section == 0:
            turned, *sent = call(body, [left, cell, plane, *halo], 0, [turned_shape, *messages])
        else:
            landed, *sent = call(
                body, [left, cell, plane, turned, pick, from_low_y, from_high_y], 0, [shape(coming, columns), *messages]
            )
        xp, xm, yp, ym = (x.astype(jnp.float16) for x in sent)
        from_low_x = shifted(xp, "gx", 1)
        from_high_x = shifted(xm, "gx", -1)
        out = call(
            functools.partial(advance, section, widths, more),
            ([targets[section - 1], landed] if section else [])
            + [cells, plane, turned, state]
            + ([velocity, *halo] if more else []),
            1 if section else 0,
            [shape(count + SPARE if section else count, columns)]
            + ([plane_shape, turned_shape] if more else []),
        )
        state, plane, turned = out if more else (out, None, None)
        from_low_y = shifted(
            jnp.concatenate([yp, from_low_x[SEGMENT : 2 * SEGMENT], from_high_x[2 * SEGMENT :]], axis=0), "gy", 1
        )
        from_high_y = shifted(
            jnp.concatenate([ym, from_low_x[2 * SEGMENT :], from_high_x[SEGMENT : 2 * SEGMENT]], axis=0), "gy", -1
        )
        from_low_y, from_high_y = from_low_y.astype(jnp.float32), from_high_y.astype(jnp.float32)
        out = call(
            functools.partial(settle, section, more),
            [targets[section]]
            + ([slot[section + 1]] if more else [])
            + [state, from_low_x[:SEGMENT].astype(jnp.float32), from_high_x[:SEGMENT].astype(jnp.float32)]
            + ([rows, leave, arrive] if more else []),
            2 if more else 1,
            [shape(count + SPARE, columns)]
            + (
                [shape(leaving, columns), cell_shape, shape(leaving, coming, dtype=jnp.bfloat16)]
                if more
                else []
            ),
            [pltpu.VMEM((2 * CAP, columns), jnp.float32)] + ([gathered] if more else []),
        )
        state, left, cell, pick = out if more else (out, None, None, None)
    state = call(
        land,
        [targets[sections - 1], state, from_low_y],
        1,
        [shape(count + SPARE, columns)],
        [pltpu.VMEM((3 * CAP, columns), jnp.float32)],
    )
    return pl.pallas_call(
        finish,
        out_shape=shape(count, columns),
        in_specs=[smem, vmem, vmem],
        out_specs=hbm,
        scratch_shapes=[
            pltpu.VMEM((count + SPARE, columns), jnp.float32),
            pltpu.VMEM((3 * CAP, columns), jnp.float32),
            pltpu.SemaphoreType.DMA((PIECES,)),
        ],
        compiler_params=params,
        name="finish",
    )(targets[sections - 1], state, from_high_y)


def solution(mesh):
    return jax.shard_map(
        local,
        mesh=mesh,
        in_specs=(
            P(("gx", "gy"), None),
            P(None, None, "gx", "gy", None),
            P(None, None, ("gx", "gy")),
            P(None, ("gx", "gy")),
            P(None, "gx", "gy", None),
        ),
        out_specs=P(("gx", "gy"), None),
        check_vma=False,
    )
```

```python
import functools

import jax
import jax.numpy as jnp
from jax import lax
from jax.experimental import pallas as pl
from jax.experimental.pallas import tpu as pltpu
from jax.sharding import PartitionSpec as P


CAP = 64
DIRS = 8
GAMMA = (8.0 / 15.0, 5.0 / 12.0, 3.0 / 4.0)
ZETA = (0.0, -17.0 / 60.0, -5.0 / 12.0)
SEGMENTS = (0, 4, 6, 1, 5, 7, 2, 3)
FROM_XP = (1, None, None)
FROM_XM = (0, None, None)
FROM_YP = (3, 5, 6)
FROM_YM = (2, 7, 4)
TAIL = 8
FIRST = 6
SEGMENT = CAP + TAIL
RANGE = 2.0**15
SHRINK = 2.0**-10
SECOND = 2.0**11
TINY = 2.0**-14
NUDGE = 0.75 * 2.0**-12
SPARE = 8
UNROLL = 16
VMEM_BYTES = 16 * 2**20
LANES = 256
PIECES = 1


def shifted(x, axis, by):
    size = lax.axis_size(axis)
    return lax.ppermute(x, axis, [(i, (i + by) % size) for i in range(size)])


def scatter_rows(state_ref, target, arrivals):
    target_ref = target.wait()
    for ref, dirs in arrivals:
        for place, d in enumerate(dirs):
            if d is None:
                continue

            def body(t, carry, ref=ref, place=place, d=d):
                slot = target_ref[d * CAP + t]
                state_ref[pl.ds(slot, 1), :] = ref[pl.ds(place * CAP + t, 1), :]
                return carry

            lax.fori_loop(0, CAP, body, 0, unroll=UNROLL)


class Table:
    def __init__(self, source_ref, ref, sem):
        self.ref, self.copy = ref, pltpu.make_async_copy(source_ref, ref, sem)
        self.copy.start()

    def wait(self):
        self.copy.wait()
        return self.ref


def with_tables(body, count, *refs):
    sems = refs[-1]
    tables = [Table(refs[n], refs[n - count - 1], sems.at[n]) for n in range(count)]
    body(*tables, *refs[count : len(refs) - count - 1])


def gather_rows(slot, *pairs):
    slot_ref = slot.wait()

    def body(t, carry):
        slot = slot_ref[t]
        for out_ref, from_ref in pairs:
            out_ref[pl.ds(t, 1), :] = from_ref[pl.ds(slot, 1), :]
        return carry

    lax.fori_loop(0, slot_ref.shape[0], body, 0, unroll=UNROLL)


def hat(base, frac, length):
    steps = lax.broadcasted_iota(jnp.int32, (length, base.shape[1]), 0) - base
    return jnp.where(steps == 0, 1.0 - frac, jnp.where(steps == 1, frac, 0.0))


def eleven_bits(value):
    wide = value * 8193.0
    return wide - (wide - value)


def encoded(rows):
    value = rows * RANGE
    code = eleven_bits(value)
    lane = lax.broadcasted_iota(jnp.int32, rows.shape, 1)
    return jnp.where(lane < FIRST, 0.0, jnp.where(value >= code, code, -code))


def encoded_first(columns):
    value = columns * SHRINK
    high = jnp.where(jnp.abs(value) < TINY, (value + 0.75) - 0.75, eleven_bits(value))
    return high, (value - high) * SECOND


def first_columns(message_ref, place):
    stop = place * SEGMENT + CAP
    tail = message_ref[stop : stop + TAIL, :]
    return (tail[:, 0:CAP] + tail[:, CAP:] * (1.0 / SECOND)) * (1.0 / SHRINK)


def decode(segments, out_ref):
    columns = jnp.concatenate([first_columns(ref, place) for ref, place in segments], axis=1)
    for n, (ref, place) in enumerate(segments):
        code = ref[place * SEGMENT : place * SEGMENT + CAP, :]
        scale = jnp.where(code < 0.0, (1.0 - NUDGE) / RANGE, (1.0 + NUDGE) / RANGE)
        out_ref[n * CAP : (n + 1) * CAP, :] = jnp.abs(code) * scale
    out_ref[0 : len(segments) * CAP, 0:FIRST] = columns.T[:, 0:FIRST]


def split_wide(value):
    high = value.astype(jnp.bfloat16)
    return high, value - high.astype(jnp.float32)


def split(weight):
    high = weight.astype(jnp.bfloat16)
    return high, (weight - high.astype(jnp.float32)).astype(jnp.bfloat16)


def advanced(section, turned, cell, plane, rim, widths):
    width_x, width_y, depth = widths
    lanes = cell.shape[1]
    frac, before = turned[0:3], turned[3:6]
    cx, cy, cz = cell[0:1], cell[1:2], cell[2:3]
    fx, fy, fz = frac[0:1], frac[1:2], frac[2:3]
    wx = hat(cx, fx, width_x)
    wy = hat(cy, fy, width_y)
    wz = hat(cz, fz, depth)
    x_low = jnp.where(cx == -1, 1.0 - fx, 0.0)
    x_high = jnp.where(cx == width_x - 1, fx, 0.0)
    y_low = jnp.where(cy == -1, 1.0 - fy, 0.0)
    y_high = jnp.where(cy == width_y - 1, fy, 0.0)
    inner = (wx[:, None, :] * wy[None, :, :]).reshape(width_x * width_y, lanes)
    corners = [x_low * y_low, x_high * y_low, x_low * y_high, x_high * y_high]
    pad = rim.shape[1] // 2 - 2 * (width_x + width_y) - 4
    edge = jnp.concatenate(
        [x_low * wy, x_high * wy, y_low * wx, y_high * wx, *corners, jnp.zeros((pad, lanes), jnp.float32)], axis=0
    )
    high, low = split(inner)
    columns = jnp.dot(plane, high, preferred_element_type=jnp.float32)
    columns += jnp.dot(plane, low, preferred_element_type=jnp.float32)
    columns += jnp.dot(rim, jnp.concatenate(split(edge), axis=0), preferred_element_type=jnp.float32)
    speed = jnp.concatenate(
        [jnp.sum(columns[k * depth : (k + 1) * depth] * wz, axis=0, keepdims=True) for k in range(3)], axis=0
    )
    moved = frac + GAMMA[section] * speed + ZETA[section] * before
    return jnp.concatenate([moved, speed, jnp.zeros((2, lanes), jnp.float32)], axis=0)


def turn_rim(section, halo, out_ref):
    low_x, high_x, low_y, high_y = halo
    width_x, width_y, depth = low_y.shape[2] - 2, low_x.shape[2], low_x.shape[3]
    pad = out_ref.shape[1] // 2 - 2 * (width_x + width_y)
    spot = lax.broadcasted_iota(jnp.int32, (pad, depth), 0)
    for k in range(3):
        corners = jnp.zeros((pad, depth), jnp.float32)
        for n, (ref, row) in enumerate(
            ((low_y, width_x), (low_y, width_x + 1), (high_y, width_x), (high_y, width_x + 1))
        ):
            value = ref[section, k, row : row + 1, :].astype(jnp.float32)
            corners = jnp.where(spot == n, value, corners)
        rim = jnp.concatenate(
            [
                low_x[section, k],
                high_x[section, k],
                low_y[section, k, 0:width_x, :],
                high_y[section, k, 0:width_x, :],
                corners.astype(out_ref.dtype),
            ],
            axis=0,
        )
        turned = rim.T
        out_ref[k * depth : (k + 1) * depth, :] = jnp.concatenate([turned, turned], axis=1)


def turn_plane(velocity_ref, section, out_ref):
    width_x, width_y, depth = velocity_ref.shape[2:]
    for k in range(3):
        plane = velocity_ref[section, k].reshape(width_x * width_y, depth)
        out_ref[k * depth : (k + 1) * depth, :] = plane.T


def turned_row(row):
    return jnp.broadcast_to(row, (8, row.shape[1])).T[:, 0:1]


def fetch(*refs):
    sources, (state_ref, cells_ref) = refs[:5], refs[5:7]
    low_ref, high_ref, rows_ref, leave_ref, target_ref = refs[7:12]
    sections = cells_ref.shape[0]
    plane_refs, refs = refs[12 : 12 + sections], refs[12 + sections :]
    pick_refs, (velocity_ref, slots_ref, counts_ref, sems) = refs[:-4], refs[-4:]
    copies = [
        pltpu.make_async_copy(src, dst, sems.at[n])
        for n, (src, dst) in enumerate(
            zip(sources, (velocity_ref, slots_ref, counts_ref, cells_ref, state_ref))
        )
    ]
    for copy in copies:
        copy.start()
    _, parts, count = cells_ref.shape
    width_y = velocity_ref.shape[3]
    leaving = leave_ref.shape[2]

    copies[1].wait()
    copies[2].wait()
    place = lax.broadcasted_iota(jnp.int32, (DIRS, leaving), 1)
    start = lax.broadcasted_iota(jnp.int32, (DIRS, leaving), 0) * CAP
    spread = jnp.where((place >= start) & (place < start + CAP), 1.0, 0.0)
    tally = jnp.concatenate(
        [counts_ref[s, 0].astype(jnp.float32) for s in range(sections)]
        + [jnp.zeros((-sections % 8, DIRS), jnp.float32)],
        axis=0,
    )
    limit = jnp.dot(tally, spread, preferred_element_type=jnp.float32).astype(jnp.int32)
    within = lax.broadcasted_iota(jnp.int32, (1, leaving), 1) % CAP
    arrives = []
    for s in range(sections):
        order = slots_ref[s : s + 1, 0:leaving]
        target = jnp.where(within < limit[s : s + 1], order, count)
        target_ref[s] = target
        leave_ref[s] = jnp.concatenate([order[:, d * CAP : (d + 1) * CAP] for d in SEGMENTS], axis=1)
        arrive = jnp.concatenate([target[:, d * CAP : (d + 1) * CAP] for d in FROM_YP + FROM_YM], axis=1)
        arrives.append(arrive.astype(jnp.float32))
    copies[0].wait()
    for s in range(sections):
        for k in range(3):
            block = velocity_ref[s, k].astype(jnp.float32)
            low_ref[s, k] = block[:, 0, :].astype(low_ref.dtype)
            high_ref[s, k] = block[:, width_y - 1, :].astype(low_ref.dtype)
    for s, plane_ref in enumerate(plane_refs):
        turn_plane(velocity_ref, s, plane_ref)
    copies[3].wait()
    flat = jnp.concatenate(
        [cells_ref[s].astype(jnp.float32) for s in range(sections)]
        + [jnp.zeros((-sections * parts % 8, count), jnp.float32)],
        axis=0,
    )
    rows_ref[:, 0 : flat.shape[0]] = flat.T
    for s in range(1, sections):
        pick_ref, turned_pick_ref, keep_ref = pick_refs[3 * (s - 1) : 3 * s]
        leave, arrive = leave_ref[s].astype(jnp.float32), arrives[s - 1]
        pick = jnp.where(turned_row(leave) == arrive, 1.0, 0.0)
        pick_ref[...] = pick.astype(pick_ref.dtype)
        turned_pick_ref[...] = jnp.where(turned_row(arrive) == leave, 1.0, 0.0).astype(pick_ref.dtype)
        keep_ref[...] = jnp.broadcast_to(1.0 - jnp.max(pick, axis=1, keepdims=True), keep_ref.shape)
    copies[4].wait()


def own_cells(section, part_ref, cell_ref):
    parts = cell_ref.shape[0]
    cell_ref[...] = part_ref[...].T[section * parts : (section + 1) * parts].astype(jnp.int32)


def first(slot, rows_ref, state_ref, code_ref, columns_ref, cell_ref, left_ref, part_ref):
    gather_rows(slot, (left_ref, state_ref), (part_ref, rows_ref))
    own_cells(0, part_ref, cell_ref)
    rows = left_ref[...]
    code_ref[...] = encoded(rows)
    columns_ref[...] = rows.T[0:TAIL]


def depart(section, widths, *refs):
    code_ref, columns_ref, cell_ref, plane_ref = refs[:4]
    leaving = code_ref.shape[0]
    codes, columns = code_ref[...], columns_ref[...]
    if section == 0:
        halo, turned_ref, outs = refs[4:8], refs[8], refs[9:]
        turn_rim(section, halo, turned_ref)
    else:
        turned_ref, pick_ref, turned_pick_ref, c_ref, d_ref = refs[4:9]
        outs = refs[9:]
        came = [(ref, place) for ref in (c_ref, d_ref) for place in range(3)]
        arrived = jnp.concatenate([first_columns(ref, place) for ref, place in came], axis=1)
        high, rest = split_wide(arrived)
        middle, low = split(rest)
        parts = [part.astype(jnp.float32) for part in (high, middle, low)]
        put = jnp.dot(
            jnp.concatenate(parts, axis=0).astype(jnp.bfloat16),
            turned_pick_ref[...],
            preferred_element_type=jnp.float32,
        )
        for n in range(len(parts)):
            columns += put[n * TAIL : (n + 1) * TAIL]
        arrived = jnp.concatenate(
            [ref[place * SEGMENT : place * SEGMENT + CAP, :] for ref, place in came], axis=0
        )
        put = jnp.dot(
            pick_ref[...], jnp.concatenate(split(arrived), axis=1), preferred_element_type=jnp.float32
        )
        width = arrived.shape[1]
        codes += put[:, 0:width] + put[:, width:]
    outs = [(ref, place) for ref in outs for place in range(ref.shape[0] // SEGMENT)]
    for n, (ref, place) in enumerate(outs):
        ref[place * SEGMENT : place * SEGMENT + CAP, :] = codes[n * CAP : (n + 1) * CAP]
    for start in range(0, leaving, LANES):
        new = advanced(
            section,
            columns[:, start : start + LANES],
            cell_ref[:, start : start + LANES],
            plane_ref[...],
            turned_ref[...],
            widths,
        )
        high, low = encoded_first(new)
        for n in range(LANES // CAP):
            ref, place = outs[start // CAP + n]
            own = slice(n * CAP, (n + 1) * CAP)
            stop = place * SEGMENT + CAP
            ref[stop : stop + TAIL, :] = jnp.concatenate([high[:, own], low[:, own]], axis=1)


def advance(section, widths, halos, *refs):
    if section:
        target, c_ref, d_ref, *refs, work_ref, landed_ref = refs
    cells_ref, plane_ref, turned_ref, state_ref, *refs = refs
    halo, (out_ref, *turned_refs) = refs[:halos], refs[halos:]
    if section:
        work_ref[...] = state_ref[...]
        decode([(ref, place) for ref in (c_ref, d_ref) for place in range(3)], landed_ref)
        scatter_rows(work_ref, target, ((landed_ref, FROM_YP + FROM_YM),))
        state_ref = work_ref
    count = cells_ref.shape[2]
    for start in range(0, count, LANES):
        rows = state_ref[start : start + LANES, :]
        cell = cells_ref[section, :, start : start + LANES]
        new = advanced(section, rows.T, cell, plane_ref[...], turned_ref[...], widths)
        out_ref[start : start + LANES, :] = rows
        out_ref[start : start + LANES, 0:6] = new.T[:, 0:6]
    for n, next_ref in enumerate(turned_refs):
        turn_rim(section + 1 + n, halo, next_ref)


def settle(section, more, target, *refs):
    if more:
        slot, old_ref, a_ref, b_ref, rows_ref, keep_ref = refs[:6]
        state_ref, code_ref, columns_ref, cell_ref = refs[6:10]
        landed_ref, left_ref, part_ref = refs[10:]
    else:
        old_ref, a_ref, b_ref, state_ref, landed_ref = refs
    decode([(a_ref, 0), (b_ref, 0)], landed_ref)
    state_ref[0 : old_ref.shape[0], :] = old_ref[...]
    scatter_rows(state_ref, target, ((landed_ref, (FROM_XP[0], FROM_XM[0])),))
    if more:
        gather_rows(slot, (left_ref, state_ref), (part_ref, rows_ref))
        own_cells(section + 1, part_ref, cell_ref)
        rows = left_ref[...] * keep_ref[...]
        code_ref[...] = encoded(rows)
        columns_ref[...] = rows.T[0:TAIL]


def land(target, old_ref, c_ref, state_ref, landed_ref):
    state_ref[...] = old_ref[...]
    decode([(c_ref, place) for place in range(3)], landed_ref)
    scatter_rows(state_ref, target, ((landed_ref, FROM_YP),))


def finish(target, old_ref, d_ref, out_hbm, work_ref, landed_ref, sems):
    count = out_hbm.shape[0]
    work_ref[...] = old_ref[...]
    decode([(d_ref, place) for place in range(3)], landed_ref)
    scatter_rows(work_ref, target, ((landed_ref, FROM_YM),))
    step = count // PIECES
    copies = [
        pltpu.make_async_copy(
            work_ref.at[pl.ds(n * step, step), :], out_hbm.at[pl.ds(n * step, step), :], sems.at[n]
        )
        for n in range(PIECES)
    ]
    for copy in copies:
        copy.start()
    for copy in copies:
        copy.wait()


def local(state, velocity, cells, slots, counts):
    sections = velocity.shape[0]
    width_x, width_y, depth = widths = velocity.shape[2:]
    count, columns = state.shape
    leaving = DIRS * CAP
    coming = CAP * (len(FROM_YP) + len(FROM_YM))
    vmem = pl.BlockSpec(memory_space=pltpu.VMEM)
    hbm = pl.BlockSpec(memory_space=pltpu.HBM)
    params = pltpu.CompilerParams(vmem_limit_bytes=VMEM_BYTES)

    def shape(*dims, dtype=jnp.float32):
        return jax.ShapeDtypeStruct(dims, dtype)

    def call(body, operands, tables, outs, scratch=(), spec=vmem, out_spec=vmem):
        single = len(outs) == 1
        wanted = [pltpu.SMEM(x.shape, x.dtype) for x in operands[:tables]]
        if tables:
            scratch = [*scratch, *wanted, pltpu.SemaphoreType.DMA((tables,))]
            body = functools.partial(with_tables, body, tables)
        return pl.pallas_call(
            body,
            out_shape=outs[0] if single else outs,
            in_specs=[spec] * len(operands),
            out_specs=out_spec if single else [out_spec] * len(outs),
            scratch_shapes=scratch,
            compiler_params=params,
        )(*operands)

    plane_shape = shape(3 * depth, width_x * width_y, dtype=velocity.dtype)
    edge_shape = shape(sections, 3, width_x, depth, dtype=velocity.dtype)
    cell_shape = shape(3, leaving, dtype=jnp.int32)
    pick_shapes = [
        shape(leaving, coming, dtype=jnp.bfloat16),
        shape(coming, leaving, dtype=jnp.bfloat16),
        shape(leaving, columns),
    ]
    gathered = pltpu.VMEM((leaving, columns), jnp.float32)

    low_x = shifted(velocity[:, :, width_x - 1], "gx", 1)
    high_x = shifted(velocity[:, :, 0], "gx", -1)
    sources = (velocity, slots, counts, cells, state)
    state, cells, bottom, top, rows, leave, target, *rest = call(
        fetch,
        [pltpu.with_memory_space_constraint(x, pltpu.HBM) for x in sources],
        0,
        [
            shape(*state.shape),
            shape(*cells.shape, dtype=cells.dtype),
            edge_shape,
            edge_shape,
            shape(count, columns),
            shape(sections, 1, leaving, dtype=jnp.int32),
            shape(sections, 1, leaving, dtype=jnp.int32),
            *[plane_shape] * sections,
            *pick_shapes * (sections - 1),
        ],
        [
            pltpu.VMEM(velocity.shape, velocity.dtype),
            pltpu.VMEM(slots.shape, slots.dtype),
            pltpu.VMEM(counts.shape, counts.dtype),
            pltpu.SemaphoreType.DMA((5,)),
        ],
        hbm,
    )
    planes, picks = rest[:sections], rest[sections:]
    low_y = shifted(jnp.concatenate([top, low_x[:, :, width_y - 1 :], high_x[:, :, width_y - 1 :]], axis=2), "gy", 1)
    high_y = shifted(jnp.concatenate([bottom, low_x[:, :, :1], high_x[:, :, :1]], axis=2), "gy", -1)
    halo = [low_x, high_x, low_y, high_y]
    used = 2 * (width_x + width_y) + 4
    turned_shape = shape(3 * depth, 2 * (used + -used % 16), dtype=velocity.dtype)
    targets = [target[section].reshape(leaving) for section in range(sections)]
    slot = [leave[section].reshape(leaving) for section in range(sections)]

    ahead = [shape(leaving, columns), shape(TAIL, leaving), cell_shape]
    left = call(first, [slot[0], rows, state], 1, ahead, [gathered] * 2)
    messages = [shape(3 * SEGMENT, columns)] * 2 + [shape(SEGMENT, columns)] * 2
    for section in range(sections):
        more = section + 1 < sections
        body = functools.partial(depart, section, widths)
        if section == 0:
            first_turned, *sent = call(body, [*left, planes[0], *halo], 0, [turned_shape, *messages])
        else:
            sent = call(
                body, [*left, planes[section], turned[section], *pick[:2], from_low_y, from_high_y], 0, messages
            )
        xp, xm, yp, ym = (x.astype(jnp.float16) for x in sent)
        from_low_x = shifted(xp, "gx", 1)
        from_high_x = shifted(xm, "gx", -1)
        extra = halo if section == 0 else []
        if section == 0:
            turned = [first_turned]
        out = call(
            functools.partial(advance, section, widths, len(extra)),
            ([targets[section - 1], from_low_y, from_high_y] if section else [])
            + [cells, planes[section], turned[section], state, *extra],
            1 if section else 0,
            [shape(count, columns)]
            + ([turned_shape] * (sections - 1) if extra else []),
            [pltpu.VMEM((n, columns), jnp.float32) for n in (count + SPARE, coming)] if section else [],
        )
        if extra and sections > 1:
            state, *more_turned = out
            turned += more_turned
        else:
            state = out
        from_low_y = shifted(
            jnp.concatenate([yp, from_low_x[SEGMENT : 2 * SEGMENT], from_high_x[2 * SEGMENT :]], axis=0), "gy", 1
        )
        from_high_y = shifted(
            jnp.concatenate([ym, from_low_x[2 * SEGMENT :], from_high_x[SEGMENT : 2 * SEGMENT]], axis=0), "gy", -1
        )
        from_low_y, from_high_y = from_low_y.astype(jnp.float32), from_high_y.astype(jnp.float32)
        pick = picks[3 * section : 3 * section + 3]
        out = call(
            functools.partial(settle, section, more),
            [targets[section]]
            + ([slot[section + 1]] if more else [])
            + [state, from_low_x[:SEGMENT].astype(jnp.float32), from_high_x[:SEGMENT].astype(jnp.float32)]
            + ([rows, pick[2]] if more else []),
            2 if more else 1,
            [shape(count + SPARE, columns)]
            + (ahead if more else []),
            [pltpu.VMEM((2 * CAP, columns), jnp.float32)] + ([gathered] * 2 if more else []),
        )
        if more:
            state, *left = out
        else:
            state = out
    state = call(
        land,
        [targets[sections - 1], state, from_low_y],
        1,
        [shape(count + SPARE, columns)],
        [pltpu.VMEM((3 * CAP, columns), jnp.float32)],
    )
    return call(
        finish,
        [targets[sections - 1], state, from_high_y],
        1,
        [shape(count, columns)],
        [
            pltpu.VMEM((count + SPARE, columns), jnp.float32),
            pltpu.VMEM((3 * CAP, columns), jnp.float32),
            pltpu.SemaphoreType.DMA((PIECES,)),
        ],
        out_spec=hbm,
    )


def solution(mesh):
    return jax.shard_map(
        local,
        mesh=mesh,
        in_specs=(
            P(("gx", "gy"), None),
            P(None, None, "gx", "gy", None),
            P(None, None, ("gx", "gy")),
            P(None, ("gx", "gy")),
            P(None, "gx", "gy", None),
        ),
        out_specs=P(("gx", "gy"), None),
        check_vma=False,
    )
```

```python
import functools

import jax
import jax.numpy as jnp
from jax import lax
from jax.experimental import pallas as pl
from jax.experimental.pallas import tpu as pltpu
from jax.sharding import PartitionSpec as P


CAP = 64
DIRS = 8
GAMMA = (8.0 / 15.0, 5.0 / 12.0, 3.0 / 4.0)
ZETA = (0.0, -17.0 / 60.0, -5.0 / 12.0)
SEGMENTS = (0, 4, 6, 1, 5, 7, 2, 3)
FROM_XP = (1, None, None)
FROM_XM = (0, None, None)
FROM_YP = (3, 5, 6)
FROM_YM = (2, 7, 4)
TAIL = 8
FIRST = 6
SEGMENT = CAP + TAIL
RANGE = 2.0**15
SHRINK = 2.0**-10
SECOND = 2.0**11
TINY = 2.0**-14
NUDGE = 0.75 * 2.0**-12
SPARE = 8
UNROLL = 64
SHORT = 32
VMEM_BYTES = 16 * 2**20
LANES = 256
PIECES = 1


def shifted(x, axis, by):
    size = lax.axis_size(axis)
    return lax.ppermute(x, axis, [(i, (i + by) % size) for i in range(size)])


def scatter_rows(state_ref, target, arrivals, unroll=CAP):
    target_ref = target.wait()
    for ref, dirs in arrivals:
        for place, d in enumerate(dirs):
            if d is None:
                continue

            def body(t, carry, ref=ref, place=place, d=d):
                slot = target_ref[d * CAP + t]
                state_ref[pl.ds(slot, 1), :] = ref[pl.ds(place * CAP + t, 1), :]
                return carry

            lax.fori_loop(0, CAP, body, 0, unroll=unroll)


class Table:
    def __init__(self, source_ref, ref, sem):
        self.ref, self.copy = ref, pltpu.make_async_copy(source_ref, ref, sem)
        self.copy.start()

    def wait(self):
        self.copy.wait()
        return self.ref


def with_tables(body, count, *refs):
    sems = refs[-1]
    tables = [Table(refs[n], refs[n - count - 1], sems.at[n]) for n in range(count)]
    body(*tables, *refs[count : len(refs) - count - 1])


def gather_rows(slot, *pairs):
    slot_ref = slot.wait()

    def body(t, carry):
        slot = slot_ref[t]
        for out_ref, from_ref in pairs:
            out_ref[pl.ds(t, 1), :] = from_ref[pl.ds(slot, 1), :]
        return carry

    lax.fori_loop(0, slot_ref.shape[0], body, 0, unroll=UNROLL)


def hat(base, frac, length):
    steps = lax.broadcasted_iota(jnp.int32, (length, base.shape[1]), 0) - base
    return jnp.where(steps == 0, 1.0 - frac, jnp.where(steps == 1, frac, 0.0))


def eleven_bits(value):
    wide = value * 8193.0
    return wide - (wide - value)


def encoded(rows):
    value = rows * RANGE
    code = eleven_bits(value)
    lane = lax.broadcasted_iota(jnp.int32, rows.shape, 1)
    return jnp.where(lane < FIRST, 0.0, jnp.where(value >= code, code, -code))


def encoded_first(columns):
    value = columns * SHRINK
    high = jnp.where(jnp.abs(value) < TINY, (value + 0.75) - 0.75, eleven_bits(value))
    return high, (value - high) * SECOND


def first_columns(message_ref, place):
    stop = place * SEGMENT + CAP
    tail = message_ref[stop : stop + TAIL, :]
    return (tail[:, 0:CAP] + tail[:, CAP:] * (1.0 / SECOND)) * (1.0 / SHRINK)


def decode(segments, out_ref):
    columns = jnp.concatenate([first_columns(ref, place) for ref, place in segments], axis=1)
    for n, (ref, place) in enumerate(segments):
        code = ref[place * SEGMENT : place * SEGMENT + CAP, :]
        scale = jnp.where(code < 0.0, (1.0 - NUDGE) / RANGE, (1.0 + NUDGE) / RANGE)
        out_ref[n * CAP : (n + 1) * CAP, :] = jnp.abs(code) * scale
    out_ref[0 : len(segments) * CAP, 0:FIRST] = columns.T[:, 0:FIRST]


def split_wide(value):
    high = value.astype(jnp.bfloat16)
    return high, value - high.astype(jnp.float32)


def split(weight):
    high = weight.astype(jnp.bfloat16)
    return high, (weight - high.astype(jnp.float32)).astype(jnp.bfloat16)


def advanced(section, turned, cell, plane, rim, widths):
    width_x, width_y, depth = widths
    lanes = cell.shape[1]
    frac, before = turned[0:3], turned[3:6]
    cx, cy, cz = cell[0:1], cell[1:2], cell[2:3]
    fx, fy, fz = frac[0:1], frac[1:2], frac[2:3]
    wx = hat(cx, fx, width_x)
    wy = hat(cy, fy, width_y)
    wz = hat(cz, fz, depth)
    x_low = jnp.where(cx == -1, 1.0 - fx, 0.0)
    x_high = jnp.where(cx == width_x - 1, fx, 0.0)
    y_low = jnp.where(cy == -1, 1.0 - fy, 0.0)
    y_high = jnp.where(cy == width_y - 1, fy, 0.0)
    inner = (wx[:, None, :] * wy[None, :, :]).reshape(width_x * width_y, lanes)
    corners = [x_low * y_low, x_high * y_low, x_low * y_high, x_high * y_high]
    pad = rim.shape[1] // 2 - 2 * (width_x + width_y) - 4
    edge = jnp.concatenate(
        [x_low * wy, x_high * wy, y_low * wx, y_high * wx, *corners, jnp.zeros((pad, lanes), jnp.float32)], axis=0
    )
    high, low = split(inner)
    columns = jnp.dot(plane, high, preferred_element_type=jnp.float32)
    columns += jnp.dot(plane, low, preferred_element_type=jnp.float32)
    columns += jnp.dot(rim, jnp.concatenate(split(edge), axis=0), preferred_element_type=jnp.float32)
    speed = jnp.concatenate(
        [jnp.sum(columns[k * depth : (k + 1) * depth] * wz, axis=0, keepdims=True) for k in range(3)], axis=0
    )
    moved = frac + GAMMA[section] * speed + ZETA[section] * before
    return jnp.concatenate([moved, speed, jnp.zeros((2, lanes), jnp.float32)], axis=0)


def turn_rim(section, halo, out_ref):
    low_x, high_x, low_y, high_y = halo
    width_x, width_y, depth = low_y.shape[2] - 2, low_x.shape[2], low_x.shape[3]
    pad = out_ref.shape[1] // 2 - 2 * (width_x + width_y)
    spot = lax.broadcasted_iota(jnp.int32, (pad, depth), 0)
    for k in range(3):
        corners = jnp.zeros((pad, depth), jnp.float32)
        for n, (ref, row) in enumerate(
            ((low_y, width_x), (low_y, width_x + 1), (high_y, width_x), (high_y, width_x + 1))
        ):
            value = ref[section, k, row : row + 1, :].astype(jnp.float32)
            corners = jnp.where(spot == n, value, corners)
        rim = jnp.concatenate(
            [
                low_x[section, k],
                high_x[section, k],
                low_y[section, k, 0:width_x, :],
                high_y[section, k, 0:width_x, :],
                corners.astype(out_ref.dtype),
            ],
            axis=0,
        )
        turned = rim.T
        out_ref[k * depth : (k + 1) * depth, :] = jnp.concatenate([turned, turned], axis=1)


def turn_plane(velocity_ref, section, out_ref):
    width_x, width_y, depth = velocity_ref.shape[2:]
    for k in range(3):
        plane = velocity_ref[section, k].reshape(width_x * width_y, depth)
        out_ref[k * depth : (k + 1) * depth, :] = plane.T


def turned_row(row):
    return jnp.broadcast_to(row, (8, row.shape[1])).T[:, 0:1]


def fetch(*refs):
    sources, (state_ref, cells_ref) = refs[:5], refs[5:7]
    low_ref, high_ref, rows_ref, leave_ref, target_ref = refs[7:12]
    sections = cells_ref.shape[0]
    plane_refs, refs = refs[12 : 12 + sections], refs[12 + sections :]
    pick_refs, (velocity_ref, slots_ref, counts_ref, sems) = refs[:-4], refs[-4:]
    copies = [
        pltpu.make_async_copy(src, dst, sems.at[n])
        for n, (src, dst) in enumerate(
            zip(sources, (velocity_ref, slots_ref, counts_ref, cells_ref, state_ref))
        )
    ]
    for copy in copies:
        copy.start()
    _, parts, count = cells_ref.shape
    width_y = velocity_ref.shape[3]
    leaving = leave_ref.shape[2]

    copies[1].wait()
    copies[2].wait()
    place = lax.broadcasted_iota(jnp.int32, (DIRS, leaving), 1)
    start = lax.broadcasted_iota(jnp.int32, (DIRS, leaving), 0) * CAP
    spread = jnp.where((place >= start) & (place < start + CAP), 1.0, 0.0)
    tally = jnp.concatenate(
        [counts_ref[s, 0].astype(jnp.float32) for s in range(sections)]
        + [jnp.zeros((-sections % 8, DIRS), jnp.float32)],
        axis=0,
    )
    limit = jnp.dot(tally, spread, preferred_element_type=jnp.float32).astype(jnp.int32)
    within = lax.broadcasted_iota(jnp.int32, (1, leaving), 1) % CAP
    arrives = []
    for s in range(sections):
        order = slots_ref[s : s + 1, 0:leaving]
        target = jnp.where(within < limit[s : s + 1], order, count)
        target_ref[s] = target
        leave_ref[s] = jnp.concatenate([order[:, d * CAP : (d + 1) * CAP] for d in SEGMENTS], axis=1)
        arrive = jnp.concatenate([target[:, d * CAP : (d + 1) * CAP] for d in FROM_YP + FROM_YM], axis=1)
        arrives.append(arrive.astype(jnp.float32))
    copies[0].wait()
    for s in range(sections):
        for k in range(3):
            block = velocity_ref[s, k].astype(jnp.float32)
            low_ref[s, k] = block[:, 0, :].astype(low_ref.dtype)
            high_ref[s, k] = block[:, width_y - 1, :].astype(low_ref.dtype)
    for s, plane_ref in enumerate(plane_refs):
        turn_plane(velocity_ref, s, plane_ref)
    copies[3].wait()
    flat = jnp.concatenate(
        [cells_ref[s].astype(jnp.float32) for s in range(sections)]
        + [jnp.zeros((-sections * parts % 8, count), jnp.float32)],
        axis=0,
    )
    rows_ref[:, 0 : flat.shape[0]] = flat.T
    for s in range(1, sections):
        pick_ref, turned_pick_ref, keep_ref = pick_refs[3 * (s - 1) : 3 * s]
        leave, arrive = leave_ref[s].astype(jnp.float32), arrives[s - 1]
        pick = jnp.where(turned_row(leave) == arrive, 1.0, 0.0)
        pick_ref[...] = pick.astype(pick_ref.dtype)
        turned_pick_ref[...] = jnp.where(turned_row(arrive) == leave, 1.0, 0.0).astype(pick_ref.dtype)
        keep_ref[...] = jnp.broadcast_to(1.0 - jnp.max(pick, axis=1, keepdims=True), keep_ref.shape)
    copies[4].wait()


def own_cells(section, part_ref, cell_ref):
    parts = cell_ref.shape[0]
    cell_ref[...] = part_ref[...].T[section * parts : (section + 1) * parts].astype(jnp.int32)


def first(slot, rows_ref, state_ref, code_ref, columns_ref, cell_ref, left_ref, part_ref):
    gather_rows(slot, (left_ref, state_ref), (part_ref, rows_ref))
    own_cells(0, part_ref, cell_ref)
    rows = left_ref[...]
    code_ref[...] = encoded(rows)
    columns_ref[...] = rows.T[0:TAIL]


def depart(section, widths, *refs):
    code_ref, columns_ref, cell_ref, plane_ref = refs[:4]
    leaving = code_ref.shape[0]
    codes, columns = code_ref[...], columns_ref[...]
    if section == 0:
        halo, turned_ref, outs = refs[4:8], refs[8], refs[9:]
        turn_rim(section, halo, turned_ref)
    else:
        turned_ref, pick_ref, turned_pick_ref, c_ref, d_ref = refs[4:9]
        outs = refs[9:]
        came = [(ref, place) for ref in (c_ref, d_ref) for place in range(3)]
        arrived = jnp.concatenate([first_columns(ref, place) for ref, place in came], axis=1)
        high, rest = split_wide(arrived)
        middle, low = split(rest)
        parts = [part.astype(jnp.float32) for part in (high, middle, low)]
        put = jnp.dot(
            jnp.concatenate(parts, axis=0).astype(jnp.bfloat16),
            turned_pick_ref[...],
            preferred_element_type=jnp.float32,
        )
        for n in range(len(parts)):
            columns += put[n * TAIL : (n + 1) * TAIL]
        arrived = jnp.concatenate(
            [ref[place * SEGMENT : place * SEGMENT + CAP, :] for ref, place in came], axis=0
        )
        put = jnp.dot(
            pick_ref[...], jnp.concatenate(split(arrived), axis=1), preferred_element_type=jnp.float32
        )
        width = arrived.shape[1]
        codes += put[:, 0:width] + put[:, width:]
    outs = [(ref, place) for ref in outs for place in range(ref.shape[0] // SEGMENT)]
    for n, (ref, place) in enumerate(outs):
        ref[place * SEGMENT : place * SEGMENT + CAP, :] = codes[n * CAP : (n + 1) * CAP]
    for start in range(0, leaving, LANES):
        new = advanced(
            section,
            columns[:, start : start + LANES],
            cell_ref[:, start : start + LANES],
            plane_ref[...],
            turned_ref[...],
            widths,
        )
        high, low = encoded_first(new)
        for n in range(LANES // CAP):
            ref, place = outs[start // CAP + n]
            own = slice(n * CAP, (n + 1) * CAP)
            stop = place * SEGMENT + CAP
            ref[stop : stop + TAIL, :] = jnp.concatenate([high[:, own], low[:, own]], axis=1)


def advance(section, widths, halos, *refs):
    if section:
        target, c_ref, d_ref, *refs, work_ref, landed_ref = refs
    cells_ref, plane_ref, turned_ref, state_ref, *refs = refs
    halo, (out_ref, *turned_refs) = refs[:halos], refs[halos:]
    if section:
        work_ref[...] = state_ref[...]
        decode([(ref, place) for ref in (c_ref, d_ref) for place in range(3)], landed_ref)
        scatter_rows(work_ref, target, ((landed_ref, FROM_YP + FROM_YM),), SHORT)
        state_ref = work_ref
    count = cells_ref.shape[2]
    for start in range(0, count, LANES):
        rows = state_ref[start : start + LANES, :]
        cell = cells_ref[section, :, start : start + LANES]
        new = advanced(section, rows.T, cell, plane_ref[...], turned_ref[...], widths)
        out_ref[start : start + LANES, :] = rows
        out_ref[start : start + LANES, 0:6] = new.T[:, 0:6]
    for n, next_ref in enumerate(turned_refs):
        turn_rim(section + 1 + n, halo, next_ref)


def settle(section, more, target, *refs):
    if more:
        slot, old_ref, a_ref, b_ref, rows_ref, keep_ref = refs[:6]
        state_ref, code_ref, columns_ref, cell_ref = refs[6:10]
        landed_ref, left_ref, part_ref = refs[10:]
    else:
        old_ref, a_ref, b_ref, state_ref, landed_ref = refs
    decode([(a_ref, 0), (b_ref, 0)], landed_ref)
    state_ref[0 : old_ref.shape[0], :] = old_ref[...]
    scatter_rows(state_ref, target, ((landed_ref, (FROM_XP[0], FROM_XM[0])),))
    if more:
        gather_rows(slot, (left_ref, state_ref), (part_ref, rows_ref))
        own_cells(section + 1, part_ref, cell_ref)
        rows = left_ref[...] * keep_ref[...]
        code_ref[...] = encoded(rows)
        columns_ref[...] = rows.T[0:TAIL]


def land(target, old_ref, c_ref, state_ref, landed_ref):
    state_ref[...] = old_ref[...]
    decode([(c_ref, place) for place in range(3)], landed_ref)
    scatter_rows(state_ref, target, ((landed_ref, FROM_YP),))


def finish(target, old_ref, d_ref, out_hbm, work_ref, landed_ref, sems):
    count = out_hbm.shape[0]
    work_ref[...] = old_ref[...]
    decode([(d_ref, place) for place in range(3)], landed_ref)
    scatter_rows(work_ref, target, ((landed_ref, FROM_YM),))
    step = count // PIECES
    copies = [
        pltpu.make_async_copy(
            work_ref.at[pl.ds(n * step, step), :], out_hbm.at[pl.ds(n * step, step), :], sems.at[n]
        )
        for n in range(PIECES)
    ]
    for copy in copies:
        copy.start()
    for copy in copies:
        copy.wait()


def local(state, velocity, cells, slots, counts):
    sections = velocity.shape[0]
    width_x, width_y, depth = widths = velocity.shape[2:]
    count, columns = state.shape
    leaving = DIRS * CAP
    coming = CAP * (len(FROM_YP) + len(FROM_YM))
    vmem = pl.BlockSpec(memory_space=pltpu.VMEM)
    hbm = pl.BlockSpec(memory_space=pltpu.HBM)
    params = pltpu.CompilerParams(vmem_limit_bytes=VMEM_BYTES)

    def shape(*dims, dtype=jnp.float32):
        return jax.ShapeDtypeStruct(dims, dtype)

    def call(body, operands, tables, outs, scratch=(), spec=vmem, out_spec=vmem):
        single = len(outs) == 1
        wanted = [pltpu.SMEM(x.shape, x.dtype) for x in operands[:tables]]
        if tables:
            scratch = [*scratch, *wanted, pltpu.SemaphoreType.DMA((tables,))]
            body = functools.partial(with_tables, body, tables)
        return pl.pallas_call(
            body,
            out_shape=outs[0] if single else outs,
            in_specs=[spec] * len(operands),
            out_specs=out_spec if single else [out_spec] * len(outs),
            scratch_shapes=scratch,
            compiler_params=params,
        )(*operands)

    plane_shape = shape(3 * depth, width_x * width_y, dtype=velocity.dtype)
    edge_shape = shape(sections, 3, width_x, depth, dtype=velocity.dtype)
    cell_shape = shape(3, leaving, dtype=jnp.int32)
    pick_shapes = [
        shape(leaving, coming, dtype=jnp.bfloat16),
        shape(coming, leaving, dtype=jnp.bfloat16),
        shape(leaving, columns),
    ]
    gathered = pltpu.VMEM((leaving, columns), jnp.float32)

    low_x = shifted(velocity[:, :, width_x - 1], "gx", 1)
    high_x = shifted(velocity[:, :, 0], "gx", -1)
    sources = (velocity, slots, counts, cells, state)
    state, cells, bottom, top, rows, leave, target, *rest = call(
        fetch,
        [pltpu.with_memory_space_constraint(x, pltpu.HBM) for x in sources],
        0,
        [
            shape(*state.shape),
            shape(*cells.shape, dtype=cells.dtype),
            edge_shape,
            edge_shape,
            shape(count, columns),
            shape(sections, 1, leaving, dtype=jnp.int32),
            shape(sections, 1, leaving, dtype=jnp.int32),
            *[plane_shape] * sections,
            *pick_shapes * (sections - 1),
        ],
        [
            pltpu.VMEM(velocity.shape, velocity.dtype),
            pltpu.VMEM(slots.shape, slots.dtype),
            pltpu.VMEM(counts.shape, counts.dtype),
            pltpu.SemaphoreType.DMA((5,)),
        ],
        hbm,
    )
    planes, picks = rest[:sections], rest[sections:]
    low_y = shifted(jnp.concatenate([top, low_x[:, :, width_y - 1 :], high_x[:, :, width_y - 1 :]], axis=2), "gy", 1)
    high_y = shifted(jnp.concatenate([bottom, low_x[:, :, :1], high_x[:, :, :1]], axis=2), "gy", -1)
    halo = [low_x, high_x, low_y, high_y]
    used = 2 * (width_x + width_y) + 4
    turned_shape = shape(3 * depth, 2 * (used + -used % 16), dtype=velocity.dtype)
    targets = [target[section].reshape(leaving) for section in range(sections)]
    slot = [leave[section].reshape(leaving) for section in range(sections)]

    ahead = [shape(leaving, columns), shape(TAIL, leaving), cell_shape]
    left = call(first, [slot[0], rows, state], 1, ahead, [gathered] * 2)
    messages = [shape(3 * SEGMENT, columns)] * 2 + [shape(SEGMENT, columns)] * 2
    for section in range(sections):
        more = section + 1 < sections
        body = functools.partial(depart, section, widths)
        if section == 0:
            first_turned, *sent = call(body, [*left, planes[0], *halo], 0, [turned_shape, *messages])
        else:
            sent = call(
                body, [*left, planes[section], turned[section], *pick[:2], from_low_y, from_high_y], 0, messages
            )
        xp, xm, yp, ym = (x.astype(jnp.float16) for x in sent)
        from_low_x = shifted(xp, "gx", 1)
        from_high_x = shifted(xm, "gx", -1)
        extra = halo if section == 0 else []
        if section == 0:
            turned = [first_turned]
        out = call(
            functools.partial(advance, section, widths, len(extra)),
            ([targets[section - 1], from_low_y, from_high_y] if section else [])
            + [cells, planes[section], turned[section], state, *extra],
            1 if section else 0,
            [shape(count, columns)]
            + ([turned_shape] * (sections - 1) if extra else []),
            [pltpu.VMEM((n, columns), jnp.float32) for n in (count + SPARE, coming)] if section else [],
        )
        if extra and sections > 1:
            state, *more_turned = out
            turned += more_turned
        else:
            state = out
        from_low_y = shifted(
            jnp.concatenate([yp, from_low_x[SEGMENT : 2 * SEGMENT], from_high_x[2 * SEGMENT :]], axis=0), "gy", 1
        )
        from_high_y = shifted(
            jnp.concatenate([ym, from_low_x[2 * SEGMENT :], from_high_x[SEGMENT : 2 * SEGMENT]], axis=0), "gy", -1
        )
        from_low_y, from_high_y = from_low_y.astype(jnp.float32), from_high_y.astype(jnp.float32)
        pick = picks[3 * section : 3 * section + 3]
        out = call(
            functools.partial(settle, section, more),
            [targets[section]]
            + ([slot[section + 1]] if more else [])
            + [state, from_low_x[:SEGMENT].astype(jnp.float32), from_high_x[:SEGMENT].astype(jnp.float32)]
            + ([rows, pick[2]] if more else []),
            2 if more else 1,
            [shape(count + SPARE, columns)]
            + (ahead if more else []),
            [pltpu.VMEM((2 * CAP, columns), jnp.float32)] + ([gathered] * 2 if more else []),
        )
        if more:
            state, *left = out
        else:
            state = out
    state = call(
        land,
        [targets[sections - 1], state, from_low_y],
        1,
        [shape(count + SPARE, columns)],
        [pltpu.VMEM((3 * CAP, columns), jnp.float32)],
    )
    return call(
        finish,
        [targets[sections - 1], state, from_high_y],
        1,
        [shape(count, columns)],
        [
            pltpu.VMEM((count + SPARE, columns), jnp.float32),
            pltpu.VMEM((3 * CAP, columns), jnp.float32),
            pltpu.SemaphoreType.DMA((PIECES,)),
        ],
        out_spec=hbm,
    )


def solution(mesh):
    return jax.shard_map(
        local,
        mesh=mesh,
        in_specs=(
            P(("gx", "gy"), None),
            P(None, None, "gx", "gy", None),
            P(None, None, ("gx", "gy")),
            P(None, ("gx", "gy")),
            P(None, "gx", "gy", None),
        ),
        out_specs=P(("gx", "gy"), None),
        check_vma=False,
    )
```

```python
import functools

import jax
import jax.numpy as jnp
from jax import lax
from jax.experimental import pallas as pl
from jax.experimental.pallas import tpu as pltpu
from jax.sharding import PartitionSpec as P


CAP = 64
DIRS = 8
GAMMA = (8.0 / 15.0, 5.0 / 12.0, 3.0 / 4.0)
ZETA = (0.0, -17.0 / 60.0, -5.0 / 12.0)
SEGMENTS = (0, 4, 6, 1, 5, 7, 2, 3)
FROM_XP = (1, None, None)
FROM_XM = (0, None, None)
FROM_YP = (3, 5, 6)
FROM_YM = (2, 7, 4)
TAIL = 8
FIRST = 6
SEGMENT = CAP + TAIL
RANGE = 2.0**15
SHRINK = 2.0**-10
SECOND = 2.0**11
TINY = 2.0**-14
NUDGE = 0.75 * 2.0**-12
SPARE = 8
UNROLL = 64
SHORT = 64
VMEM_BYTES = 16 * 2**20
LANES = 256
LATER = (0, 2, 4)
PIECES = 1


def shifted(x, axis, by):
    size = lax.axis_size(axis)
    return lax.ppermute(x, axis, [(i, (i + by) % size) for i in range(size)])


def scatter_rows(state_ref, target, arrivals, unroll=CAP):
    target_ref = target.wait()
    for ref, dirs in arrivals:
        for place, d in enumerate(dirs):
            if d is None:
                continue

            def body(t, carry, ref=ref, place=place, d=d):
                slot = target_ref[d * CAP + t]
                state_ref[pl.ds(slot, 1), :] = ref[pl.ds(place * CAP + t, 1), :]
                return carry

            lax.fori_loop(0, CAP, body, 0, unroll=unroll)


class Table:
    def __init__(self, source_ref, ref, sem):
        self.ref, self.copy = ref, pltpu.make_async_copy(source_ref, ref, sem)
        self.copy.start()

    def wait(self):
        self.copy.wait()
        return self.ref


def with_tables(body, count, *refs):
    sems = refs[-1]
    tables = [Table(refs[n], refs[n - count - 1], sems.at[n]) for n in range(count)]
    body(*tables, *refs[count : len(refs) - count - 1])


def gather_rows(slot, *pairs):
    slot_ref = slot.wait()

    def body(t, carry):
        slot = slot_ref[t]
        for out_ref, from_ref in pairs:
            out_ref[pl.ds(t, 1), :] = from_ref[pl.ds(slot, 1), :]
        return carry

    lax.fori_loop(0, slot_ref.shape[0], body, 0, unroll=UNROLL)


def hat(base, frac, length):
    steps = lax.broadcasted_iota(jnp.int32, (length, base.shape[1]), 0) - base
    return jnp.where(steps == 0, 1.0 - frac, jnp.where(steps == 1, frac, 0.0))


def eleven_bits(value):
    wide = value * 8193.0
    return wide - (wide - value)


def encoded(rows):
    value = rows * RANGE
    code = eleven_bits(value)
    lane = lax.broadcasted_iota(jnp.int32, rows.shape, 1)
    return jnp.where(lane < FIRST, 0.0, jnp.where(value >= code, code, -code))


def encoded_first(columns):
    value = columns * SHRINK
    high = jnp.where(jnp.abs(value) < TINY, (value + 0.75) - 0.75, eleven_bits(value))
    return high, (value - high) * SECOND


def first_columns(message_ref, place):
    stop = place * SEGMENT + CAP
    tail = message_ref[stop : stop + TAIL, :]
    return (tail[:, 0:CAP] + tail[:, CAP:] * (1.0 / SECOND)) * (1.0 / SHRINK)


def decode(segments, out_ref):
    columns = jnp.concatenate([first_columns(ref, place) for ref, place in segments], axis=1)
    for n, (ref, place) in enumerate(segments):
        code = ref[place * SEGMENT : place * SEGMENT + CAP, :]
        scale = jnp.where(code < 0.0, (1.0 - NUDGE) / RANGE, (1.0 + NUDGE) / RANGE)
        out_ref[n * CAP : (n + 1) * CAP, :] = jnp.abs(code) * scale
    out_ref[0 : len(segments) * CAP, 0:FIRST] = columns.T[:, 0:FIRST]


def split_wide(value):
    high = value.astype(jnp.bfloat16)
    return high, value - high.astype(jnp.float32)


def split(weight):
    high = weight.astype(jnp.bfloat16)
    return high, (weight - high.astype(jnp.float32)).astype(jnp.bfloat16)


def advanced(section, turned, cell, plane, rim, widths):
    width_x, width_y, depth = widths
    lanes = cell.shape[1]
    frac, before = turned[0:3], turned[3:6]
    cx, cy, cz = cell[0:1], cell[1:2], cell[2:3]
    fx, fy, fz = frac[0:1], frac[1:2], frac[2:3]
    wx = hat(cx, fx, width_x)
    wy = hat(cy, fy, width_y)
    wz = hat(cz, fz, depth)
    x_low = jnp.where(cx == -1, 1.0 - fx, 0.0)
    x_high = jnp.where(cx == width_x - 1, fx, 0.0)
    y_low = jnp.where(cy == -1, 1.0 - fy, 0.0)
    y_high = jnp.where(cy == width_y - 1, fy, 0.0)
    inner = (wx[:, None, :] * wy[None, :, :]).reshape(width_x * width_y, lanes)
    corners = [x_low * y_low, x_high * y_low, x_low * y_high, x_high * y_high]
    pad = rim.shape[1] // 2 - 2 * (width_x + width_y) - 4
    edge = jnp.concatenate(
        [x_low * wy, x_high * wy, y_low * wx, y_high * wx, *corners, jnp.zeros((pad, lanes), jnp.float32)], axis=0
    )
    high, low = split(inner)
    columns = jnp.dot(plane, high, preferred_element_type=jnp.float32)
    columns += jnp.dot(plane, low, preferred_element_type=jnp.float32)
    columns += jnp.dot(rim, jnp.concatenate(split(edge), axis=0), preferred_element_type=jnp.float32)
    speed = jnp.concatenate(
        [jnp.sum(columns[k * depth : (k + 1) * depth] * wz, axis=0, keepdims=True) for k in range(3)], axis=0
    )
    moved = frac + GAMMA[section] * speed + ZETA[section] * before
    return jnp.concatenate([moved, speed, jnp.zeros((2, lanes), jnp.float32)], axis=0)


def turn_rim(section, halo, out_ref):
    low_x, high_x, low_y, high_y = halo
    width_x, width_y, depth = low_y.shape[2] - 2, low_x.shape[2], low_x.shape[3]
    pad = out_ref.shape[1] // 2 - 2 * (width_x + width_y)
    spot = lax.broadcasted_iota(jnp.int32, (pad, depth), 0)
    for k in range(3):
        corners = jnp.zeros((pad, depth), jnp.float32)
        for n, (ref, row) in enumerate(
            ((low_y, width_x), (low_y, width_x + 1), (high_y, width_x), (high_y, width_x + 1))
        ):
            value = ref[section, k, row : row + 1, :].astype(jnp.float32)
            corners = jnp.where(spot == n, value, corners)
        rim = jnp.concatenate(
            [
                low_x[section, k],
                high_x[section, k],
                low_y[section, k, 0:width_x, :],
                high_y[section, k, 0:width_x, :],
                corners.astype(out_ref.dtype),
            ],
            axis=0,
        )
        turned = rim.T
        out_ref[k * depth : (k + 1) * depth, :] = jnp.concatenate([turned, turned], axis=1)


def turn_plane(velocity_ref, section, out_ref):
    width_x, width_y, depth = velocity_ref.shape[2:]
    for k in range(3):
        plane = velocity_ref[section, k].reshape(width_x * width_y, depth)
        out_ref[k * depth : (k + 1) * depth, :] = plane.T


def turned_row(row):
    return jnp.broadcast_to(row, (8, row.shape[1])).T[:, 0:1]


def fetch(*refs):
    sources, (state_ref, cells_ref) = refs[:5], refs[5:7]
    low_ref, high_ref, rows_ref, leave_ref, target_ref = refs[7:12]
    sections = cells_ref.shape[0]
    plane_refs, refs = refs[12 : 12 + sections], refs[12 + sections :]
    pick_refs, (velocity_ref, slots_ref, counts_ref, sems) = refs[:-4], refs[-4:]
    copies = [
        pltpu.make_async_copy(src, dst, sems.at[n])
        for n, (src, dst) in enumerate(
            zip(sources, (velocity_ref, slots_ref, counts_ref, cells_ref, state_ref))
        )
    ]
    for copy in copies:
        copy.start()
    _, parts, count = cells_ref.shape
    width_y = velocity_ref.shape[3]
    leaving = leave_ref.shape[2]

    copies[1].wait()
    copies[2].wait()
    place = lax.broadcasted_iota(jnp.int32, (DIRS, leaving), 1)
    start = lax.broadcasted_iota(jnp.int32, (DIRS, leaving), 0) * CAP
    spread = jnp.where((place >= start) & (place < start + CAP), 1.0, 0.0)
    tally = jnp.concatenate(
        [counts_ref[s, 0].astype(jnp.float32) for s in range(sections)]
        + [jnp.zeros((-sections % 8, DIRS), jnp.float32)],
        axis=0,
    )
    limit = jnp.dot(tally, spread, preferred_element_type=jnp.float32).astype(jnp.int32)
    within = lax.broadcasted_iota(jnp.int32, (1, leaving), 1) % CAP
    arrives = []
    for s in range(sections):
        order = slots_ref[s : s + 1, 0:leaving]
        target = jnp.where(within < limit[s : s + 1], order, count)
        target_ref[s] = target
        leave_ref[s] = jnp.concatenate([order[:, d * CAP : (d + 1) * CAP] for d in SEGMENTS], axis=1)
        arrive = jnp.concatenate([target[:, d * CAP : (d + 1) * CAP] for d in FROM_YP + FROM_YM], axis=1)
        arrives.append(arrive.astype(jnp.float32))
    copies[0].wait()
    for s in range(sections):
        for k in range(3):
            block = velocity_ref[s, k].astype(jnp.float32)
            low_ref[s, k] = block[:, 0, :].astype(low_ref.dtype)
            high_ref[s, k] = block[:, width_y - 1, :].astype(low_ref.dtype)
    for s, plane_ref in enumerate(plane_refs):
        turn_plane(velocity_ref, s, plane_ref)
    copies[3].wait()
    flat = jnp.concatenate(
        [cells_ref[s].astype(jnp.float32) for s in range(sections)]
        + [jnp.zeros((-sections * parts % 8, count), jnp.float32)],
        axis=0,
    )
    rows_ref[:, 0 : flat.shape[0]] = flat.T
    for s in range(1, sections):
        pick_ref, turned_pick_ref, keep_ref = pick_refs[3 * (s - 1) : 3 * s]
        leave, arrive = leave_ref[s].astype(jnp.float32), arrives[s - 1]
        pick = jnp.where(turned_row(leave) == arrive, 1.0, 0.0)
        pick_ref[...] = pick.astype(pick_ref.dtype)
        turned_pick_ref[...] = jnp.where(turned_row(arrive) == leave, 1.0, 0.0).astype(pick_ref.dtype)
        keep_ref[...] = jnp.broadcast_to(1.0 - jnp.max(pick, axis=1, keepdims=True), keep_ref.shape)
    copies[4].wait()


def own_cells(section, part_ref, cell_ref):
    parts = cell_ref.shape[0]
    cell_ref[...] = part_ref[...].T[section * parts : (section + 1) * parts].astype(jnp.int32)


def first(slot, rows_ref, state_ref, code_ref, columns_ref, cell_ref, left_ref, part_ref):
    gather_rows(slot, (left_ref, state_ref), (part_ref, rows_ref))
    own_cells(0, part_ref, cell_ref)
    rows = left_ref[...]
    code_ref[...] = encoded(rows)
    columns_ref[...] = rows.T[0:TAIL]


def depart(section, widths, *refs):
    code_ref, columns_ref, cell_ref, plane_ref = refs[:4]
    leaving = code_ref.shape[0]
    codes, columns = code_ref[...], columns_ref[...]
    if section == 0:
        halo, turned_ref, outs = refs[4:8], refs[8], refs[9:]
        turn_rim(section, halo, turned_ref)
    else:
        turned_ref, pick_ref, turned_pick_ref, c_ref, d_ref = refs[4:9]
        outs = refs[9:]
        came = [(ref, place) for ref in (c_ref, d_ref) for place in range(3)]
        arrived = jnp.concatenate([first_columns(ref, place) for ref, place in came], axis=1)
        high, rest = split_wide(arrived)
        middle, low = split(rest)
        parts = [part.astype(jnp.float32) for part in (high, middle, low)]
        put = jnp.dot(
            jnp.concatenate(parts, axis=0).astype(jnp.bfloat16),
            turned_pick_ref[...],
            preferred_element_type=jnp.float32,
        )
        for n in range(len(parts)):
            columns += put[n * TAIL : (n + 1) * TAIL]
        arrived = jnp.concatenate(
            [ref[place * SEGMENT : place * SEGMENT + CAP, :] for ref, place in came], axis=0
        )
        put = jnp.dot(
            pick_ref[...], jnp.concatenate(split(arrived), axis=1), preferred_element_type=jnp.float32
        )
        width = arrived.shape[1]
        codes += put[:, 0:width] + put[:, width:]
    outs = [(ref, place) for ref in outs for place in range(ref.shape[0] // SEGMENT)]
    for n, (ref, place) in enumerate(outs):
        ref[place * SEGMENT : place * SEGMENT + CAP, :] = codes[n * CAP : (n + 1) * CAP]
    for start in range(0, leaving, LANES):
        new = advanced(
            section,
            columns[:, start : start + LANES],
            cell_ref[:, start : start + LANES],
            plane_ref[...],
            turned_ref[...],
            widths,
        )
        high, low = encoded_first(new)
        for n in range(LANES // CAP):
            ref, place = outs[start // CAP + n]
            own = slice(n * CAP, (n + 1) * CAP)
            stop = place * SEGMENT + CAP
            ref[stop : stop + TAIL, :] = jnp.concatenate([high[:, own], low[:, own]], axis=1)


def advance(section, widths, halos, *refs):
    if section:
        target, c_ref, d_ref, *refs, work_ref, landed_ref = refs
    cells_ref, plane_ref, turned_ref, state_ref, *refs = refs
    halo, (out_ref, *turned_refs) = refs[:halos], refs[halos:]
    if section:
        work_ref[...] = state_ref[...]
        decode([(ref, place) for ref in (c_ref, d_ref) for place in range(3)], landed_ref)
        scatter_rows(work_ref, target, ((landed_ref, FROM_YP + FROM_YM),), SHORT)
        state_ref = work_ref
    count = cells_ref.shape[2]
    for start in range(0, count, LANES):
        rows = state_ref[start : start + LANES, :]
        out_ref[start : start + LANES, :] = rows
        if start < LATER[section] * LANES:
            continue
        cell = cells_ref[section, :, start : start + LANES]
        new = advanced(section, rows.T, cell, plane_ref[...], turned_ref[...], widths)
        out_ref[start : start + LANES, 0:6] = new.T[:, 0:6]
    for n, next_ref in enumerate(turned_refs):
        turn_rim(section + 1 + n, halo, next_ref)


def settle(section, widths, more, target, *refs):
    if more:
        slot, *refs = refs
    if LATER[section]:
        cells_ref, plane_ref, turned_ref, *refs = refs
    if more:
        old_ref, a_ref, b_ref, rows_ref, keep_ref = refs[:5]
        state_ref, code_ref, columns_ref, cell_ref = refs[5:9]
        landed_ref, left_ref, part_ref = refs[9:]
    else:
        old_ref, a_ref, b_ref, state_ref, landed_ref = refs
    decode([(a_ref, 0), (b_ref, 0)], landed_ref)
    state_ref[0 : old_ref.shape[0], :] = old_ref[...]
    for start in range(0, LATER[section] * LANES, LANES):
        columns = old_ref[start : start + LANES, :].T
        cell = cells_ref[section, :, start : start + LANES]
        new = advanced(section, columns, cell, plane_ref[...], turned_ref[...], widths)
        state_ref[start : start + LANES, 0:6] = new.T[:, 0:6]
    scatter_rows(state_ref, target, ((landed_ref, (FROM_XP[0], FROM_XM[0])),))
    if more:
        gather_rows(slot, (left_ref, state_ref), (part_ref, rows_ref))
        own_cells(section + 1, part_ref, cell_ref)
        rows = left_ref[...] * keep_ref[...]
        code_ref[...] = encoded(rows)
        columns_ref[...] = rows.T[0:TAIL]


def land(target, old_ref, c_ref, state_ref, landed_ref):
    state_ref[...] = old_ref[...]
    decode([(c_ref, place) for place in range(3)], landed_ref)
    scatter_rows(state_ref, target, ((landed_ref, FROM_YP),))


def finish(target, old_ref, d_ref, out_hbm, work_ref, landed_ref, sems):
    count = out_hbm.shape[0]
    work_ref[...] = old_ref[...]
    decode([(d_ref, place) for place in range(3)], landed_ref)
    scatter_rows(work_ref, target, ((landed_ref, FROM_YM),))
    step = count // PIECES
    copies = [
        pltpu.make_async_copy(
            work_ref.at[pl.ds(n * step, step), :], out_hbm.at[pl.ds(n * step, step), :], sems.at[n]
        )
        for n in range(PIECES)
    ]
    for copy in copies:
        copy.start()
    for copy in copies:
        copy.wait()


def local(state, velocity, cells, slots, counts):
    sections = velocity.shape[0]
    width_x, width_y, depth = widths = velocity.shape[2:]
    count, columns = state.shape
    leaving = DIRS * CAP
    coming = CAP * (len(FROM_YP) + len(FROM_YM))
    vmem = pl.BlockSpec(memory_space=pltpu.VMEM)
    hbm = pl.BlockSpec(memory_space=pltpu.HBM)
    params = pltpu.CompilerParams(vmem_limit_bytes=VMEM_BYTES)

    def shape(*dims, dtype=jnp.float32):
        return jax.ShapeDtypeStruct(dims, dtype)

    def call(body, operands, tables, outs, scratch=(), spec=vmem, out_spec=vmem):
        single = len(outs) == 1
        wanted = [pltpu.SMEM(x.shape, x.dtype) for x in operands[:tables]]
        if tables:
            scratch = [*scratch, *wanted, pltpu.SemaphoreType.DMA((tables,))]
            body = functools.partial(with_tables, body, tables)
        return pl.pallas_call(
            body,
            out_shape=outs[0] if single else outs,
            in_specs=[spec] * len(operands),
            out_specs=out_spec if single else [out_spec] * len(outs),
            scratch_shapes=scratch,
            compiler_params=params,
        )(*operands)

    plane_shape = shape(3 * depth, width_x * width_y, dtype=velocity.dtype)
    edge_shape = shape(sections, 3, width_x, depth, dtype=velocity.dtype)
    cell_shape = shape(3, leaving, dtype=jnp.int32)
    pick_shapes = [
        shape(leaving, coming, dtype=jnp.bfloat16),
        shape(coming, leaving, dtype=jnp.bfloat16),
        shape(leaving, columns),
    ]
    gathered = pltpu.VMEM((leaving, columns), jnp.float32)

    low_x = shifted(velocity[:, :, width_x - 1], "gx", 1)
    high_x = shifted(velocity[:, :, 0], "gx", -1)
    sources = (velocity, slots, counts, cells, state)
    state, cells, bottom, top, rows, leave, target, *rest = call(
        fetch,
        [pltpu.with_memory_space_constraint(x, pltpu.HBM) for x in sources],
        0,
        [
            shape(*state.shape),
            shape(*cells.shape, dtype=cells.dtype),
            edge_shape,
            edge_shape,
            shape(count, columns),
            shape(sections, 1, leaving, dtype=jnp.int32),
            shape(sections, 1, leaving, dtype=jnp.int32),
            *[plane_shape] * sections,
            *pick_shapes * (sections - 1),
        ],
        [
            pltpu.VMEM(velocity.shape, velocity.dtype),
            pltpu.VMEM(slots.shape, slots.dtype),
            pltpu.VMEM(counts.shape, counts.dtype),
            pltpu.SemaphoreType.DMA((5,)),
        ],
        hbm,
    )
    planes, picks = rest[:sections], rest[sections:]
    low_y = shifted(jnp.concatenate([top, low_x[:, :, width_y - 1 :], high_x[:, :, width_y - 1 :]], axis=2), "gy", 1)
    high_y = shifted(jnp.concatenate([bottom, low_x[:, :, :1], high_x[:, :, :1]], axis=2), "gy", -1)
    halo = [low_x, high_x, low_y, high_y]
    used = 2 * (width_x + width_y) + 4
    turned_shape = shape(3 * depth, 2 * (used + -used % 16), dtype=velocity.dtype)
    targets = [target[section].reshape(leaving) for section in range(sections)]
    slot = [leave[section].reshape(leaving) for section in range(sections)]

    ahead = [shape(leaving, columns), shape(TAIL, leaving), cell_shape]
    left = call(first, [slot[0], rows, state], 1, ahead, [gathered] * 2)
    messages = [shape(3 * SEGMENT, columns)] * 2 + [shape(SEGMENT, columns)] * 2
    for section in range(sections):
        more = section + 1 < sections
        body = functools.partial(depart, section, widths)
        if section == 0:
            first_turned, *sent = call(body, [*left, planes[0], *halo], 0, [turned_shape, *messages])
        else:
            sent = call(
                body, [*left, planes[section], turned[section], *pick[:2], from_low_y, from_high_y], 0, messages
            )
        xp, xm, yp, ym = (x.astype(jnp.float16) for x in sent)
        from_low_x = shifted(xp, "gx", 1)
        from_high_x = shifted(xm, "gx", -1)
        extra = halo if section == 0 else []
        if section == 0:
            turned = [first_turned]
        out = call(
            functools.partial(advance, section, widths, len(extra)),
            ([targets[section - 1], from_low_y, from_high_y] if section else [])
            + [cells, planes[section], turned[section], state, *extra],
            1 if section else 0,
            [shape(count, columns)]
            + ([turned_shape] * (sections - 1) if extra else []),
            [pltpu.VMEM((n, columns), jnp.float32) for n in (count + SPARE, coming)] if section else [],
        )
        if extra and sections > 1:
            state, *more_turned = out
            turned += more_turned
        else:
            state = out
        from_low_y = shifted(
            jnp.concatenate([yp, from_low_x[SEGMENT : 2 * SEGMENT], from_high_x[2 * SEGMENT :]], axis=0), "gy", 1
        )
        from_high_y = shifted(
            jnp.concatenate([ym, from_low_x[2 * SEGMENT :], from_high_x[SEGMENT : 2 * SEGMENT]], axis=0), "gy", -1
        )
        from_low_y, from_high_y = from_low_y.astype(jnp.float32), from_high_y.astype(jnp.float32)
        pick = picks[3 * section : 3 * section + 3]
        out = call(
            functools.partial(settle, section, widths, more),
            [targets[section]]
            + ([slot[section + 1]] if more else [])
            + ([cells, planes[section], turned[section]] if LATER[section] else [])
            + [state, from_low_x[:SEGMENT].astype(jnp.float32), from_high_x[:SEGMENT].astype(jnp.float32)]
            + ([rows, pick[2]] if more else []),
            2 if more else 1,
            [shape(count + SPARE, columns)]
            + (ahead if more else []),
            [pltpu.VMEM((2 * CAP, columns), jnp.float32)] + ([gathered] * 2 if more else []),
        )
        if more:
            state, *left = out
        else:
            state = out
    state = call(
        land,
        [targets[sections - 1], state, from_low_y],
        1,
        [shape(count + SPARE, columns)],
        [pltpu.VMEM((3 * CAP, columns), jnp.float32)],
    )
    return call(
        finish,
        [targets[sections - 1], state, from_high_y],
        1,
        [shape(count, columns)],
        [
            pltpu.VMEM((count + SPARE, columns), jnp.float32),
            pltpu.VMEM((3 * CAP, columns), jnp.float32),
            pltpu.SemaphoreType.DMA((PIECES,)),
        ],
        out_spec=hbm,
    )


def solution(mesh):
    return jax.shard_map(
        local,
        mesh=mesh,
        in_specs=(
            P(("gx", "gy"), None),
            P(None, None, "gx", "gy", None),
            P(None, None, ("gx", "gy")),
            P(None, ("gx", "gy")),
            P(None, "gx", "gy", None),
        ),
        out_specs=P(("gx", "gy"), None),
        check_vma=False,
    )
```
